512 devices in a mesh: rows: 64 (over y, z), cols: 8 (over x, core).
Axes of the slice: x: 4, y: 8, z: 8, core: 2. Of those that a mesh axis runs over, the one named last changes fastest.
Arguments:
- residues: int32 [16384, 4096], P('rows', 'cols'), may hold values from 0 to 20, as said below
- dirichlet: float32 [9, 20], replicated, may hold values from 0.02 to 2
- mix_weight: float32 [9], replicated, may hold values from 0.05 to 1
- background: float32 [20], replicated, may hold values from 0.02 to 0.12
Outputs:
- profile: float32 [20, 4096], P(None, 'cols')
- scores: float32 [16384], P('rows')
- weights: float32 [16384], P('rows')
The draws below stay inside these ranges and needn't reach their ends.
Inputs may be any that keep to these rules, and one draw needn't show every extreme that they name: `residues`: residue codes; 20 stands for a gap.
All inputs are finite; a program needn't handle non-finite values.
Results may differ from the reference program's by a relative error of at most 0.0003.
Values sent between devices are 32-bit elements; how exact they have to be, the bound alone decides.
A program may use at most 64 MiB of HBM per device.

```python
import math
import jax
import jax.numpy as jnp
from jax import lax

L = 4096
ALPHABET = 20
COMPONENTS = 9
ITERS = 3
SEQS = 16384


def draw_residues(key, part):
    keys = jax.random.split(jax.random.fold_in(key, 11), 5)
    families = jax.random.randint(keys[0], (SEQS,), 0, 4)
    consensus = jax.random.randint(keys[1], (4, L), 0, 20)
    ancestral = jnp.take(consensus, families, axis=0)
    mutation_rate = jax.random.randint(keys[2], (SEQS, 1), 5, 80)
    chance = jax.random.randint(keys[3], (SEQS, L), 0, 100)
    mutant = jax.random.randint(keys[4], (SEQS, L), 0, 21)
    return jnp.where(chance < mutation_rate, mutant, ancestral).astype(jnp.int32)


def setup_inputs(seed: int = 0) -> dict:
    streams_of = jax.random.split(jax.random.key(seed), 5)
    return {
        "residues": draw_residues(jax.random.fold_in(streams_of[4], 71), 0),
        "dirichlet": jnp.clip(jnp.exp(jax.random.uniform(streams_of[1], (COMPONENTS, ALPHABET), jnp.float32, math.log(0.02), math.log(2.0))), 0.02, 2.0),
        "mix_weight": jnp.clip(jnp.exp(jax.random.uniform(streams_of[2], (COMPONENTS,), jnp.float32, math.log(0.05), math.log(1.0))), 0.05, 1.0),
        "background": jnp.clip(jnp.exp(jax.random.uniform(streams_of[3], (ALPHABET,), jnp.float32, math.log(0.02), math.log(0.12))), 0.02, 0.12),
    }


count_mass = 64.0
symbols = 21

def one_hot_of(row_block):
    levels = jnp.arange(symbols, dtype=jnp.int32)
    return (row_block[None, :, :] == levels[:, None, None]).astype(jnp.float32)

def mixture(frequency, dirichlet, mix_weight, background):
    strength = lax.optimization_barrier(jnp.sum(dirichlet, axis=1))
    log_prior = jnp.log(mix_weight) - jnp.log(jnp.sum(mix_weight))
    column_total = lax.optimization_barrier(jnp.sum(frequency, axis=0))
    shifted = frequency[None, :, :] + dirichlet[:, :, None]
    likelihood = lax.optimization_barrier(jnp.sum(lax.lgamma(shifted) - lax.lgamma(dirichlet)[:, :, None], axis=1))
    likelihood = likelihood + (log_prior + lax.lgamma(strength))[:, None]
    likelihood = likelihood - lax.lgamma(strength[:, None] + column_total[None, :])
    posterior = jax.nn.softmax(likelihood, axis=0)
    shares = posterior / (column_total[None, :] + strength[:, None])
    smoothed = lax.optimization_barrier(jnp.sum(shares[:, None, :] * shifted, axis=0))
    normal_bg = background / jnp.sum(background)
    return jnp.log(smoothed / normal_bg[:, None])

def split_rows(residues):
    height = math.gcd(SEQS, 512)
    return (residues.reshape(SEQS // height, height, L), height)

def weighted_counts(residues, weight_vec):
    blocks, height = split_rows(residues)
    weight_blocks = weight_vec.reshape(SEQS // height, height)

    def accumulate(running, paired):
        row_block, weight_block = paired
        added = jnp.einsum('s,asj->aj', weight_block, one_hot_of(row_block), precision=lax.Precision.HIGHEST)
        return (running + added, None)
    running, _ = lax.scan(accumulate, jnp.zeros((symbols, L), jnp.float32), (blocks, weight_blocks))
    return running

def table_sums(residues, lookup):
    blocks, height = split_rows(residues)

    def score_block(row_block):
        return jnp.einsum('asj,aj->s', one_hot_of(row_block), lookup, precision=lax.Precision.HIGHEST)
    return lax.map(score_block, blocks).reshape(SEQS)

def reference(residues, dirichlet, mix_weight, background):
    counts = weighted_counts(residues, jnp.ones((SEQS,), jnp.float32))
    present = counts > 0.5
    distinct = lax.optimization_barrier(jnp.sum(present.astype(jnp.float32), axis=0))
    inverse = jnp.where(present, 1.0 / (distinct[None, :] * jnp.maximum(counts, 1.0)), 0.0)
    henikoff = table_sums(residues, inverse) / L
    inclusion = jnp.ones((SEQS,), jnp.float32)
    for iteration in range(ITERS):
        raw_weight = henikoff * inclusion
        total_mass = jnp.sum(raw_weight)
        weights = SEQS * raw_weight / total_mass
        summed = weighted_counts(residues, raw_weight)
        frequency = count_mass * summed[:ALPHABET] / total_mass
        profile = mixture(frequency, dirichlet, mix_weight, background)
        lookup = jnp.concatenate([profile, jnp.zeros((1, L), jnp.float32)], axis=0)
        scores = table_sums(residues, lookup) / L
        if iteration + 1 < ITERS:
            center = jnp.mean(scores)
            inclusion = jax.nn.sigmoid((scores - center) * math.sqrt(L))
    return (profile, scores, weights)
```

```python
import functools
import math

import jax
import jax.numpy as jnp
from jax import lax
from jax.experimental import pallas as pl
from jax.experimental.pallas import tpu as pltpu
from jax.sharding import PartitionSpec as P

MESH = pl.DeviceIdType.MESH
ALPHABET = 20
PAIRS = 10
COMPONENTS = 9
ITERS = 3
COUNT_MASS = 64.0
NZ = 8
LANES = 128
HALF = 64
Y_ROWS = 11
S_ROWS = 17

COUNT_Z, MOVE, GATHER, Y0 = 0, 1, 2, 3
Z0 = Y0 + ITERS + 1
C0 = Z0 + ITERS + 1
EXCHANGES = C0 + ITERS + 1
ORDER = (4, 3, 5, 2, 6, 1, 7)

f32 = jnp.float32
bf16 = jnp.bfloat16


def lgamma(x):
    t = x * (x + 3.0)
    z = x + 4.0
    r = 1.0 / z
    r2 = r * r
    series = r * (1.0 / 12.0 + r2 * (-1.0 / 360.0 + r2 * (1.0 / 1260.0 - r2 * (1.0 / 1680.0))))
    return (z - 0.5) * jnp.log(z) - z + (0.9189385332046727 + series) - jnp.log(t * (t + 2.0))


def iota(shape, dim):
    return lax.broadcasted_iota(jnp.int32, shape, dim)


def low(shape):
    return iota(shape, len(shape) - 1) < HALF


def swap(v):
    return pltpu.roll(v, HALF, 1)


def fold(v):
    return v + swap(v)


def over_rows(v):
    return jnp.sum(v, axis=0, keepdims=True)


def over_lanes(v):
    return jnp.sum(v, axis=1, keepdims=True)


def pick(x, rows):
    bits = [(x & (1 << b)) != 0 for b in range(5)]
    a = [jnp.where(bits[0], rows[2 * i + 1], rows[2 * i]) for i in range(10)]
    b = [jnp.where(bits[1], a[2 * i + 1], a[2 * i]) for i in range(5)]
    c = [jnp.where(bits[2], b[1], b[0]), jnp.where(bits[2], b[3], b[2]), jnp.where(bits[2], rows[20], b[4])]
    return jnp.where(bits[4], c[2], jnp.where(bits[3], c[1], c[0]))


def packed(totals):
    first = low((8, LANES))
    rows = []
    for p in range(PAIRS):
        u, v = totals[p], totals[p + PAIRS]
        rows.append(over_rows(jnp.where(first, u, v) + swap(jnp.where(first, v, u))))
    return rows


def kernel(
    dims,
    res_hbm,
    dir_s,
    mix_s,
    bg_s,
    prof_o,
    score_o,
    weight_o,
    res_v,
    stage,
    held,
    cnt_send,
    cbuf,
    ybuf,
    zbuf,
    sbuf,
    pbuf,
    wide,
    pieces,
    val_hi,
    val_mid,
    ones1,
    ones3,
    alpha,
    base,
    strength,
    inv_bg,
    lik,
    counts,
    hen,
    inc,
    raw_s,
    score_s,
    mass_s,
    table,
    in_sem,
    ssem,
    rsem,
):
    ny, nc, seqs, length = dims
    row = lax.axis_index("rows")
    me_c = lax.axis_index("cols")
    me_y, me_z = row // NZ, row % NZ

    def peer(axis, d):
        if axis == "z":
            return (me_y * NZ + (me_z + d) % NZ, me_c)
        if axis == "y":
            return (((me_y + d) % ny) * NZ + me_z, me_c)
        return (row, (me_c + d) % nc)

    size = {"z": NZ, "y": ny, "c": nc}
    mine = {"z": me_z, "y": me_y, "c": me_c}

    barrier = pltpu.get_barrier_semaphore()
    for axis in "yzc":
        for d in range(1, size[axis]):
            pl.semaphore_signal(barrier, inc=1, device_id=peer(axis, d), device_id_type=MESH)
    load = pltpu.make_async_copy(res_hbm, res_v, in_sem)
    load.start()

    def remote(src, dst, number, axis, d):
        return pltpu.make_async_remote_copy(
            src_ref=src,
            dst_ref=dst,
            send_sem=ssem.at[number, d - 1],
            recv_sem=rsem.at[number, d - 1],
            device_id=peer(axis, d),
            device_id_type=MESH,
        )

    def distances(axis):
        n = size[axis]
        return ORDER if n == 8 else tuple(range(1, n))

    def copies(buf, rows, number, axis):
        me = mine[axis]
        own = buf.at[me, pl.ds(0, rows)]
        return [remote(own, own, number, axis, d) for d in distances(axis)]

    def begin(made):
        for copy in made:
            copy.start()

    def arrive(made):
        for copy in made:
            copy.wait_recv()

    def leave(made):
        for copy in made:
            copy.wait_send()

    def total_of(buf, axis):
        s = buf[0]
        for i in range(1, size[axis]):
            s = s + buf[i]
        return s

    row16 = iota((16, LANES), 0)
    low16 = low((16, LANES))
    load.wait()

    for zd in range(NZ):
        block = pl.ds((zd // 2) * LANES, LANES)
        a, b = res_v[0:LANES, block], res_v[LANES : 2 * LANES, block]
        first = low((LANES, LANES))
        if zd % 2 == 0:
            stage[zd] = jnp.where(first, a, swap(b))
        else:
            stage[zd] = jnp.where(first, swap(a), b)

    def count_one(zd, carry):
        def tile(t, totals):
            for u in range(4):
                at = pl.multiple_of(t * 32 + u * 8, 8)
                x = stage[zd, pl.ds(at, 8), :]
                totals = tuple(totals[a] + jnp.where(x == a, 1.0, 0.0) for a in range(ALPHABET))
            return totals

        totals = lax.fori_loop(0, 4, tile, tuple(jnp.zeros((8, LANES), f32) for _ in range(ALPHABET)))
        for p, line in enumerate(packed(totals)):
            cnt_send[zd, p : p + 1, :] = line
        return carry

    lax.fori_loop(0, NZ, count_one, 0)
    cbuf[me_z] = cnt_send[me_z]
    held[me_z] = stage[me_z]

    pl.semaphore_wait(barrier, ny + NZ + nc - 3)

    sent_counts = []
    for d in distances("z"):
        other = (me_z + d) % NZ
        sent_counts.append(
            remote(cnt_send.at[other, pl.ds(0, PAIRS)], cbuf.at[me_z, pl.ds(0, PAIRS)], COUNT_Z, "z", d)
        )
    moved = [remote(stage.at[(me_z + d) % NZ], held.at[me_z], MOVE, "z", d) for d in distances("z")]
    begin(sent_counts)
    begin(moved)

    shape1 = (16, NZ * LANES)
    hit = (iota(shape1, 0) // 2 == iota(shape1, 1) // LANES) & (
        iota(shape1, 0) % 2 == (iota(shape1, 1) % LANES) // HALF
    )
    spread = jnp.where(hit, 1.0, 0.0).astype(bf16)
    ones1[...] = spread
    for i in range(3):
        ones3[16 * i : 16 * i + 16, :] = spread
    low1 = low((1, LANES))
    for k in range(COMPONENTS):
        alpha[k] = jnp.ones((16, LANES), f32)
        for p in range(PAIRS):
            alpha[k, p : p + 1, :] = jnp.where(low1, dir_s[k, p], dir_s[k, p + PAIRS])
    inv_bg[...] = jnp.ones((16, LANES), f32)
    for p in range(PAIRS):
        inv_bg[p : p + 1, :] = jnp.where(low1, bg_s[p], bg_s[p + PAIRS])
    bg = inv_bg[...]
    inv_bg[...] = jnp.where(row16 < PAIRS, over_rows(fold(jnp.where(row16 < PAIRS, bg, 0.0))) / bg, 1.0)
    strength[...] = jnp.ones((16, LANES), f32)
    base[...] = jnp.zeros((16, LANES), f32)
    lik[...] = jnp.ones((16, LANES), f32)
    for k in range(COMPONENTS):
        al = alpha[k]
        strength[k : k + 1, :] = over_rows(fold(jnp.where(row16 < PAIRS, al, 0.0)))
        base[k : k + 1, :] = over_rows(fold(lgamma(al)))
        lik[k : k + 1, :] = jnp.where(low1, mix_s[k], mix_s[k])
    mix = lik[...]
    log_prior = jnp.log(mix) - jnp.log(over_rows(jnp.where(row16 < COMPONENTS, mix, 0.0)))
    base[...] = log_prior + lgamma(strength[...]) - base[...]

    arrive(sent_counts)
    ybuf[0, me_y] = total_of(cbuf, "z")
    ex = copies(ybuf.at[0], Y_ROWS, Y0, "y")
    begin(ex)
    arrive(ex)
    number = jnp.where(row16 < PAIRS, total_of(ybuf.at[0], "y"), 0.0)
    counts[...] = number
    gap = seqs - over_rows(fold(number))
    present = number > 0.5
    distinct = over_rows(fold(jnp.where(present, 1.0, 0.0))) + jnp.where(gap > 0.5, 1.0, 0.0)
    inverse = jnp.where(present, 1.0 / (distinct * jnp.maximum(number, 1.0)), 0.0)
    gap_inverse = jnp.where(gap > 0.5, 1.0 / (distinct * jnp.maximum(gap, 1.0)), 0.0)

    def set_table(lines, gap_line):
        other = swap(lines)
        table[0:PAIRS, :] = jnp.where(low16, lines, other)[0:PAIRS]
        table[PAIRS:ALPHABET, :] = jnp.where(low16, other, lines)[0:PAIRS]
        table[ALPHABET : ALPHABET + 1, :] = gap_line

    def sums_of_table():
        rows = [jnp.broadcast_to(table[a : a + 1, :], (16, LANES)) for a in range(ALPHABET + 1)]

        def group(g, carry):
            at = pl.multiple_of(g * 16, 16)
            for b in range(NZ):
                v = pick(held[b, pl.ds(at, 16), :], rows)
                hi = v.astype(bf16)
                val_hi[pl.ds(at, 16), b * LANES : (b + 1) * LANES] = hi
                val_mid[pl.ds(at, 16), b * LANES : (b + 1) * LANES] = (v - hi.astype(f32)).astype(bf16)
            return carry

        lax.fori_loop(0, LANES // 16, group, 0)
        nt = (((1,), (1,)), ((), ()))
        e = ones1[...]
        return lax.dot_general(e, val_hi[...], nt, preferred_element_type=f32) + lax.dot_general(
            e, val_mid[...], nt, preferred_element_type=f32
        )

    def sum_over_columns(i, part, extra):
        zbuf[i, me_z, 0:16, :] = part
        zbuf[i, me_z, 16:24, :] = extra
        ex = copies(zbuf.at[i], S_ROWS, Z0 + i, "z")
        begin(ex)
        arrive(ex)
        sbuf[i, me_c] = total_of(zbuf.at[i], "z")
        ex = copies(sbuf.at[i], S_ROWS, C0 + i, "c")
        begin(ex)
        arrive(ex)
        return total_of(sbuf.at[i], "c")

    set_table(inverse, gap_inverse)
    arrive(moved)
    hen[...] = sum_over_columns(0, sums_of_table(), jnp.zeros((8, LANES), f32))[0:16] * (1.0 / length)
    inc[...] = jnp.ones((16, LANES), f32)

    def weighted_counts(i):
        def group(g, totals):
            for b in range(NZ):
                at = pl.multiple_of(g * 8, 8)
                x = held[b, pl.ds(at, 8), :]
                w = wide[pl.ds(at, 8), b * LANES : (b + 1) * LANES]
                totals = tuple(totals[a] + jnp.where(x == a, w, 0.0) for a in range(ALPHABET))
            return totals

        totals = lax.fori_loop(0, LANES // 8, group, tuple(jnp.zeros((8, LANES), f32) for _ in range(ALPHABET)))
        for p, line in enumerate(packed(totals)):
            ybuf[i, me_y, p : p + 1, :] = line

    def mixture(frequency):
        column_total = over_rows(fold(frequency))
        for k in range(COMPONENTS):
            lik[k : k + 1, :] = over_rows(lgamma(frequency + alpha[k]))
        lam = fold(lik[...]) + base[...] - lgamma(strength[...] + column_total)
        lam = jnp.where(row16 < COMPONENTS, lam, -1e30)
        e = jnp.exp(lam - jnp.max(lam, axis=0, keepdims=True))
        shares = e / (over_rows(e) * (column_total + strength[...]))
        smoothed = jnp.zeros((16, LANES), f32)
        for k in range(COMPONENTS):
            smoothed = smoothed + shares[k : k + 1, :] * (frequency + alpha[k])
        return jnp.log(smoothed * inv_bg[...])

    gathered = copies(pbuf, PAIRS, GATHER, "z")

    def iteration(it, carry):
        i = it + 1
        raw = hen[...] * inc[...]
        raw_s[...] = raw
        hi = raw.astype(bf16)
        rest = raw - hi.astype(f32)
        mid = rest.astype(bf16)
        pieces[0:16, :] = hi
        pieces[16:32, :] = mid
        pieces[32:48, :] = (rest - mid.astype(f32)).astype(bf16)
        wide[...] = lax.dot_general(
            pieces[...], ones3[...], (((0,), (0,)), ((), ())), preferred_element_type=f32
        )
        weighted_counts(i)
        ybuf[i, me_y, PAIRS : PAIRS + 1, :] = over_rows(raw)
        ex = copies(ybuf.at[i], Y_ROWS, Y0 + i, "y")
        begin(ex)
        arrive(ex)
        whole = total_of(ybuf.at[i], "y")
        mass = over_lanes(whole[PAIRS : PAIRS + 1, :])
        mass_s[...] = jnp.broadcast_to(mass, (8, LANES))
        frequency = jnp.where(row16 < PAIRS, whole, 0.0) * (COUNT_MASS / mass)
        profile = mixture(frequency)

        @pl.when(it == ITERS - 1)
        def _():
            pbuf[me_z] = profile
            begin(gathered)

        set_table(profile, jnp.zeros((1, LANES), f32))
        share = over_rows(jnp.where(row16 < PAIRS, profile * counts[...], 0.0))
        extra = jnp.where(iota((8, LANES), 0) == 0, share, 0.0)
        done = sum_over_columns(i, sums_of_table(), extra)
        scores = done[0:16] * (1.0 / length)
        center = over_lanes(done[16:17, :]) * (1.0 / (length * seqs))
        score_s[...] = scores
        inc[...] = 1.0 / (1.0 + jnp.exp((center - scores) * math.sqrt(length)))
        return carry

    lax.fori_loop(0, ITERS, iteration, 0)

    weights = raw_s[...] * (seqs / mass_s[0:1, :])
    scores = score_s[...]
    own_w, own_s = weights[0:2], scores[0:2]
    for b in range(1, NZ):
        own_w = jnp.where(me_z == b, weights[2 * b : 2 * b + 2], own_w)
        own_s = jnp.where(me_z == b, scores[2 * b : 2 * b + 2], own_s)
    weight_o[...] = own_w
    score_o[...] = own_s

    arrive(gathered)
    for block in range(NZ // 2):
        even, odd = pbuf[2 * block], pbuf[2 * block + 1]
        at = pl.ds(block * LANES, LANES)
        prof_o[0:PAIRS, at] = jnp.where(low16, even, swap(odd))[0:PAIRS]
        prof_o[PAIRS:ALPHABET, at] = jnp.where(low16, swap(even), odd)[0:PAIRS]

    leave(sent_counts)
    leave(moved)
    leave(gathered)
    for i in range(ITERS + 1):
        leave(copies(ybuf.at[i], Y_ROWS, Y0 + i, "y"))
        leave(copies(zbuf.at[i], S_ROWS, Z0 + i, "z"))
        leave(copies(sbuf.at[i], S_ROWS, C0 + i, "c"))


def solution(mesh):
    rows, cols = mesh.shape["rows"], mesh.shape["cols"]
    ny = rows // NZ

    def body(residues, dirichlet, mix_weight, background):
        high, across = residues.shape
        dims = (ny, cols, high * rows, across * cols)
        tile = pltpu.VMEM((16, LANES), f32)
        profile, scores, weights = pl.pallas_call(
            functools.partial(kernel, dims),
            out_shape=(
                jax.ShapeDtypeStruct((ALPHABET, across), f32),
                jax.ShapeDtypeStruct((2, LANES), f32),
                jax.ShapeDtypeStruct((2, LANES), f32),
            ),
            in_specs=[
                pl.BlockSpec(memory_space=pl.ANY),
                pl.BlockSpec(memory_space=pltpu.SMEM),
                pl.BlockSpec(memory_space=pltpu.SMEM),
                pl.BlockSpec(memory_space=pltpu.SMEM),
            ],
            out_specs=[pl.BlockSpec(memory_space=pltpu.VMEM)] * 3,
            scratch_shapes=[
                pltpu.VMEM((high, across), jnp.int32),
                pltpu.VMEM((NZ, LANES, LANES), jnp.int32),
                pltpu.VMEM((NZ, LANES, LANES), jnp.int32),
                pltpu.VMEM((NZ, 16, LANES), f32),
                pltpu.VMEM((NZ, 16, LANES), f32),
                pltpu.VMEM((ITERS + 1, ny, 16, LANES), f32),
                pltpu.VMEM((ITERS + 1, NZ, 24, LANES), f32),
                pltpu.VMEM((ITERS + 1, cols, 24, LANES), f32),
                pltpu.VMEM((NZ, 16, LANES), f32),
                pltpu.VMEM((LANES, NZ * LANES), f32),
                pltpu.VMEM((48, LANES), bf16),
                pltpu.VMEM((LANES, NZ * LANES), bf16),
                pltpu.VMEM((LANES, NZ * LANES), bf16),
                pltpu.VMEM((16, NZ * LANES), bf16),
                pltpu.VMEM((48, NZ * LANES), bf16),
                pltpu.VMEM((COMPONENTS, 16, LANES), f32),
                tile,
                tile,
                tile,
                tile,
                tile,
                tile,
                tile,
                tile,
                tile,
                pltpu.VMEM((8, LANES), f32),
                pltpu.VMEM((24, LANES), f32),
                pltpu.SemaphoreType.DMA,
                pltpu.SemaphoreType.DMA((EXCHANGES, 7)),
                pltpu.SemaphoreType.DMA((EXCHANGES, 7)),
            ],
            compiler_params=pltpu.CompilerParams(collective_id=0, has_side_effects=True),
        )(residues, dirichlet, mix_weight, background)
        return profile, scores.reshape(-1), weights.reshape(-1)

    in_specs = (P("rows", "cols"), P(), P(), P())
    out_specs = (P(None, "cols"), P("rows"), P("rows"))
    return jax.shard_map(body, mesh=mesh, in_specs=in_specs, out_specs=out_specs, check_vma=False)
```

```python
import functools
import math

import jax
import jax.numpy as jnp
from jax import lax
from jax.experimental import pallas as pl
from jax.experimental.pallas import tpu as pltpu
from jax.sharding import PartitionSpec as P

MESH = pl.DeviceIdType.MESH
ALPHABET = 20
PAIRS = 10
COMPONENTS = 9
ITERS = 3
COUNT_MASS = 64.0
NZ = 8
LANES = 128
HALF = 64
Y_ROWS = 11
S_ROWS = 17

COUNT_Z, MOVE, GATHER, Y0 = 0, 1, 2, 3
Z0 = Y0 + ITERS + 1
C0 = Z0 + ITERS + 1
EXCHANGES = C0 + ITERS + 1
ORDER = (4, 3, 5, 2, 6, 1, 7)

f32 = jnp.float32
bf16 = jnp.bfloat16


def lgamma(x):
    t = x * (x + 3.0)
    z = x + 4.0
    r = 1.0 / z
    r2 = r * r
    series = r * (1.0 / 12.0 + r2 * (-1.0 / 360.0 + r2 * (1.0 / 1260.0 - r2 * (1.0 / 1680.0))))
    return (z - 0.5) * jnp.log(z) - z + (0.9189385332046727 + series) - jnp.log(t * (t + 2.0))


def iota(shape, dim):
    return lax.broadcasted_iota(jnp.int32, shape, dim)


def low(shape):
    return iota(shape, len(shape) - 1) < HALF


def swap(v):
    return pltpu.roll(v, HALF, 1)


def fold(v):
    return v + swap(v)


def over_rows(v):
    return jnp.sum(v, axis=0, keepdims=True)


def over_lanes(v):
    return jnp.sum(v, axis=1, keepdims=True)


def pick(x, rows):
    bits = [(x & (1 << b)) != 0 for b in range(5)]
    a = [jnp.where(bits[0], rows[2 * i + 1], rows[2 * i]) for i in range(10)]
    b = [jnp.where(bits[1], a[2 * i + 1], a[2 * i]) for i in range(5)]
    c = [jnp.where(bits[2], b[1], b[0]), jnp.where(bits[2], b[3], b[2]), jnp.where(bits[2], rows[20], b[4])]
    return jnp.where(bits[4], c[2], jnp.where(bits[3], c[1], c[0]))


def packed(totals):
    first = low((8, LANES))
    rows = []
    for p in range(PAIRS):
        u, v = totals[p], totals[p + PAIRS]
        rows.append(over_rows(jnp.where(first, u, v) + swap(jnp.where(first, v, u))))
    return rows


def kernel(
    dims,
    res_hbm,
    dir_hbm,
    mix_hbm,
    bg_hbm,
    prof_o,
    score_o,
    weight_o,
    dir_s,
    mix_s,
    bg_s,
    res_v,
    stage,
    held,
    cnt_send,
    cnt_lo,
    cnt_hi,
    cbuf,
    ybuf,
    zbuf,
    sbuf,
    pbuf,
    wide,
    pieces,
    val_hi,
    val_mid,
    ones1,
    ones3,
    alpha,
    base,
    strength,
    inv_bg,
    lik,
    counts,
    hen,
    inc,
    raw_s,
    score_s,
    mass_s,
    table,
    in_sem,
    small_sem,
    ssem,
    rsem,
):
    ny, nc, seqs, length = dims
    row = lax.axis_index("rows")
    me_c = lax.axis_index("cols")
    me_y, me_z = row // NZ, row % NZ

    def peer(axis, d):
        if axis == "z":
            return (me_y * NZ + (me_z + d) % NZ, me_c)
        if axis == "y":
            return (((me_y + d) % ny) * NZ + me_z, me_c)
        return (row, (me_c + d) % nc)

    size = {"z": NZ, "y": ny, "c": nc}
    mine = {"z": me_z, "y": me_y, "c": me_c}

    barrier = pltpu.get_barrier_semaphore()
    for axis in "yzc":
        for d in range(1, size[axis]):
            pl.semaphore_signal(barrier, inc=1, device_id=peer(axis, d), device_id_type=MESH)
    load = pltpu.make_async_copy(res_hbm, res_v, in_sem)
    load.start()
    small = [
        pltpu.make_async_copy(src, dst, small_sem.at[n])
        for n, (src, dst) in enumerate(((dir_hbm, dir_s), (mix_hbm, mix_s), (bg_hbm, bg_s)))
    ]
    for copy in small:
        copy.start()

    def remote(src, dst, number, axis, d):
        return pltpu.make_async_remote_copy(
            src_ref=src,
            dst_ref=dst,
            send_sem=ssem.at[number, d - 1],
            recv_sem=rsem.at[number, d - 1],
            device_id=peer(axis, d),
            device_id_type=MESH,
        )

    def distances(axis):
        n = size[axis]
        return ORDER if n == 8 else tuple(range(1, n))

    def copies(buf, rows, number, axis):
        me = mine[axis]
        own = buf.at[me, pl.ds(0, rows)]
        return [remote(own, own, number, axis, d) for d in distances(axis)]

    def begin(made):
        for copy in made:
            copy.start()

    def arrive(made):
        for copy in made:
            copy.wait_recv()

    def leave(made):
        for copy in made:
            copy.wait_send()

    def total_of(buf, axis):
        s = buf[0]
        for i in range(1, size[axis]):
            s = s + buf[i]
        return s

    row16 = iota((16, LANES), 0)
    low16 = low((16, LANES))
    load.wait()

    for zd in range(NZ):
        block = pl.ds((zd // 2) * LANES, LANES)
        a, b = res_v[0:LANES, block], res_v[LANES : 2 * LANES, block]
        first = low((LANES, LANES))
        if zd % 2 == 0:
            stage[zd] = jnp.where(first, a, swap(b))
        else:
            stage[zd] = jnp.where(first, swap(a), b)

    def count_one(zd, carry):
        fields = [jnp.zeros((8, LANES), jnp.int32) for _ in range(5)]
        for t in range(LANES // 8):
            x = stage[zd, t * 8 : t * 8 + 8, :]
            unit = jnp.left_shift(jnp.ones((8, LANES), jnp.int32), (x & 3) * 8)
            which = x >> 2
            fields = [fields[q] + jnp.where(which == q, unit, 0) for q in range(5)]
        for q in range(5):
            v = fields[q]
            for step in (4, 2, 1):
                v = v + pltpu.roll(v, step, 0)
            for r in range(4):
                p = 4 * q + r
                line = ((v >> (8 * r)) & 255).astype(f32)
                if p < PAIRS:
                    cnt_lo[p : p + 1, :] = line[0:1]
                else:
                    cnt_hi[p - PAIRS : p - PAIRS + 1, :] = line[0:1]
        u, v = cnt_lo[...], cnt_hi[...]
        cnt_send[zd] = jnp.where(low16, u, v) + swap(jnp.where(low16, v, u))
        return carry

    lax.fori_loop(0, NZ, count_one, 0)
    cbuf[me_z] = cnt_send[me_z]
    held[me_z] = stage[me_z]

    pl.semaphore_wait(barrier, ny + NZ + nc - 3)

    sent_counts = []
    for d in distances("z"):
        other = (me_z + d) % NZ
        sent_counts.append(
            remote(cnt_send.at[other, pl.ds(0, PAIRS)], cbuf.at[me_z, pl.ds(0, PAIRS)], COUNT_Z, "z", d)
        )
    moved = [remote(stage.at[(me_z + d) % NZ], held.at[me_z], MOVE, "z", d) for d in distances("z")]
    begin(sent_counts)
    begin(moved)

    for b in range(NZ):
        half = (iota((16, LANES), 1) >= HALF).astype(jnp.int32)
        spread = jnp.where(row16 == 2 * b + half, 1.0, 0.0).astype(bf16)
        ones1[:, b * LANES : (b + 1) * LANES] = spread
        for n in range(3):
            ones3[16 * n : 16 * n + 16, b * LANES : (b + 1) * LANES] = spread
    low1 = low((1, LANES))
    for copy in small:
        copy.wait()
    for k in range(COMPONENTS):
        alpha[k] = jnp.ones((16, LANES), f32)
        for p in range(PAIRS):
            alpha[k, p : p + 1, :] = jnp.where(low1, dir_s[k, p], dir_s[k, p + PAIRS])
    inv_bg[...] = jnp.ones((16, LANES), f32)
    for p in range(PAIRS):
        inv_bg[p : p + 1, :] = jnp.where(low1, bg_s[p], bg_s[p + PAIRS])
    bg = inv_bg[...]
    inv_bg[...] = jnp.where(row16 < PAIRS, over_rows(fold(jnp.where(row16 < PAIRS, bg, 0.0))) / bg, 1.0)
    strength[...] = jnp.ones((16, LANES), f32)
    base[...] = jnp.zeros((16, LANES), f32)
    lik[...] = jnp.ones((16, LANES), f32)
    for k in range(COMPONENTS):
        al = alpha[k]
        strength[k : k + 1, :] = over_rows(fold(jnp.where(row16 < PAIRS, al, 0.0)))
        base[k : k + 1, :] = over_rows(fold(lgamma(al)))
        lik[k : k + 1, :] = jnp.where(low1, mix_s[k], mix_s[k])
    mix = lik[...]
    log_prior = jnp.log(mix) - jnp.log(over_rows(jnp.where(row16 < COMPONENTS, mix, 0.0)))
    base[...] = log_prior + lgamma(strength[...]) - base[...]

    arrive(sent_counts)
    ybuf[0, me_y] = total_of(cbuf, "z")
    ex = copies(ybuf.at[0], Y_ROWS, Y0, "y")
    begin(ex)
    arrive(ex)
    number = jnp.where(row16 < PAIRS, total_of(ybuf.at[0], "y"), 0.0)
    counts[...] = number
    gap = seqs - over_rows(fold(number))
    present = number > 0.5
    distinct = over_rows(fold(jnp.where(present, 1.0, 0.0))) + jnp.where(gap > 0.5, 1.0, 0.0)
    inverse = jnp.where(present, 1.0 / (distinct * jnp.maximum(number, 1.0)), 0.0)
    gap_inverse = jnp.where(gap > 0.5, 1.0 / (distinct * jnp.maximum(gap, 1.0)), 0.0)

    def set_table(lines, gap_line):
        other = swap(lines)
        table[0:PAIRS, :] = jnp.where(low16, lines, other)[0:PAIRS]
        table[PAIRS:ALPHABET, :] = jnp.where(low16, other, lines)[0:PAIRS]
        table[ALPHABET : ALPHABET + 1, :] = gap_line

    def sums_of_table(arriving=None):
        rows = [jnp.broadcast_to(table[a : a + 1, :], (16, LANES)) for a in range(ALPHABET + 1)]

        def look_up(b, at):
            v = pick(held[b, pl.ds(at, 16), :], rows)
            hi = v.astype(bf16)
            columns = pl.ds(b * LANES if isinstance(b, int) else pl.multiple_of(b * LANES, LANES), LANES)
            val_hi[pl.ds(at, 16), columns] = hi
            val_mid[pl.ds(at, 16), columns] = (v - hi.astype(f32)).astype(bf16)

        if arriving is None:

            def group(g, carry):
                for b in range(NZ):
                    look_up(b, pl.multiple_of(g * 16, 16))
                return carry

            lax.fori_loop(0, LANES // 16, group, 0)
        else:
            for b, copy in arriving:
                if copy is not None:
                    copy.wait_recv()

                def group(g, carry):
                    for u in range(4):
                        look_up(b, pl.multiple_of(g * 64 + u * 16, 16))
                    return carry

                lax.fori_loop(0, LANES // 64, group, 0)
        nt = (((1,), (1,)), ((), ()))
        e = ones1[...]
        return lax.dot_general(e, val_hi[...], nt, preferred_element_type=f32) + lax.dot_general(
            e, val_mid[...], nt, preferred_element_type=f32
        )

    def sum_over_columns(i, part, extra):
        zbuf[i, me_z, 0:16, :] = part
        zbuf[i, me_z, 16:24, :] = extra
        ex = copies(zbuf.at[i], S_ROWS, Z0 + i, "z")
        begin(ex)
        arrive(ex)
        sbuf[i, me_c] = total_of(zbuf.at[i], "z")
        ex = copies(sbuf.at[i], S_ROWS, C0 + i, "c")
        begin(ex)
        arrive(ex)
        return total_of(sbuf.at[i], "c")

    set_table(inverse, gap_inverse)
    arriving = [(me_z, None)]
    for d, copy in zip(distances("z"), moved):
        arriving.append(((me_z + NZ - d) % NZ, copy))
    hen[...] = sum_over_columns(0, sums_of_table(arriving), jnp.zeros((8, LANES), f32))[0:16] * (1.0 / length)
    inc[...] = jnp.ones((16, LANES), f32)

    def weighted_counts(i):
        def group(g, totals):
            for b in range(NZ):
                at = pl.multiple_of(g * 8, 8)
                x = held[b, pl.ds(at, 8), :]
                w = wide[pl.ds(at, 8), b * LANES : (b + 1) * LANES]
                totals = tuple(totals[a] + jnp.where(x == a, w, 0.0) for a in range(ALPHABET))
            return totals

        totals = lax.fori_loop(0, LANES // 8, group, tuple(jnp.zeros((8, LANES), f32) for _ in range(ALPHABET)))
        for p, line in enumerate(packed(totals)):
            ybuf[i, me_y, p : p + 1, :] = line

    def mixture(frequency):
        column_total = over_rows(fold(frequency))
        for k in range(COMPONENTS):
            lik[k : k + 1, :] = over_rows(lgamma(frequency + alpha[k]))
        lam = fold(lik[...]) + base[...] - lgamma(strength[...] + column_total)
        lam = jnp.where(row16 < COMPONENTS, lam, -1e30)
        e = jnp.exp(lam - jnp.max(lam, axis=0, keepdims=True))
        shares = e / (over_rows(e) * (column_total + strength[...]))
        smoothed = jnp.zeros((16, LANES), f32)
        for k in range(COMPONENTS):
            smoothed = smoothed + shares[k : k + 1, :] * (frequency + alpha[k])
        return jnp.log(smoothed * inv_bg[...])

    gathered = copies(pbuf, PAIRS, GATHER, "z")

    def iteration(it, carry):
        i = it + 1
        raw = hen[...] * inc[...]
        raw_s[...] = raw
        part_mass = jnp.broadcast_to(over_lanes(over_rows(raw)), (1, LANES))
        hi = raw.astype(bf16)
        rest = raw - hi.astype(f32)
        mid = rest.astype(bf16)
        pieces[0:16, :] = hi
        pieces[16:32, :] = mid
        pieces[32:48, :] = (rest - mid.astype(f32)).astype(bf16)
        wide[...] = lax.dot_general(
            pieces[...], ones3[...], (((0,), (0,)), ((), ())), preferred_element_type=f32
        )
        weighted_counts(i)
        ybuf[i, me_y, PAIRS : PAIRS + 1, :] = part_mass
        ex = copies(ybuf.at[i], Y_ROWS, Y0 + i, "y")
        begin(ex)
        arrive(ex)
        whole = total_of(ybuf.at[i], "y")
        mass = whole[PAIRS : PAIRS + 1, :]
        mass_s[...] = jnp.broadcast_to(mass, (8, LANES))
        frequency = jnp.where(row16 < PAIRS, whole, 0.0) * (COUNT_MASS / mass)
        profile = mixture(frequency)

        @pl.when(it == ITERS - 1)
        def _():
            pbuf[me_z] = profile
            begin(gathered)

        set_table(profile, jnp.zeros((1, LANES), f32))
        share = over_lanes(over_rows(jnp.where(row16 < PAIRS, profile * counts[...], 0.0)))
        extra = jnp.where(iota((8, LANES), 0) == 0, share, 0.0)
        done = sum_over_columns(i, sums_of_table(), extra)
        scores = done[0:16] * (1.0 / length)
        center = done[16:17, :] * (1.0 / (length * seqs))
        score_s[...] = scores
        inc[...] = 1.0 / (1.0 + jnp.exp((center - scores) * math.sqrt(length)))
        return carry

    lax.fori_loop(0, ITERS, iteration, 0)

    weights = raw_s[...] * (seqs / mass_s[0:1, :])
    scores = score_s[...]
    own_w, own_s = weights[0:2], scores[0:2]
    for b in range(1, NZ):
        own_w = jnp.where(me_z == b, weights[2 * b : 2 * b + 2], own_w)
        own_s = jnp.where(me_z == b, scores[2 * b : 2 * b + 2], own_s)
    weight_o[...] = own_w
    score_o[...] = own_s

    arrive(gathered)
    for block in range(NZ // 2):
        even, odd = pbuf[2 * block], pbuf[2 * block + 1]
        at = pl.ds(block * LANES, LANES)
        prof_o[0:PAIRS, at] = jnp.where(low16, even, swap(odd))[0:PAIRS]
        prof_o[PAIRS:ALPHABET, at] = jnp.where(low16, swap(even), odd)[0:PAIRS]

    leave(sent_counts)
    leave(moved)
    leave(gathered)
    for i in range(ITERS + 1):
        leave(copies(ybuf.at[i], Y_ROWS, Y0 + i, "y"))
        leave(copies(zbuf.at[i], S_ROWS, Z0 + i, "z"))
        leave(copies(sbuf.at[i], S_ROWS, C0 + i, "c"))


def solution(mesh):
    rows, cols = mesh.shape["rows"], mesh.shape["cols"]
    ny = rows // NZ

    def body(residues, dirichlet, mix_weight, background):
        high, across = residues.shape
        dims = (ny, cols, high * rows, across * cols)
        tile = pltpu.VMEM((16, LANES), f32)
        profile, scores, weights = pl.pallas_call(
            functools.partial(kernel, dims),
            out_shape=(
                jax.ShapeDtypeStruct((ALPHABET, across), f32),
                jax.ShapeDtypeStruct((2, LANES), f32),
                jax.ShapeDtypeStruct((2, LANES), f32),
            ),
            in_specs=[
                pl.BlockSpec(memory_space=pl.ANY),
                pl.BlockSpec(memory_space=pl.ANY),
                pl.BlockSpec(memory_space=pl.ANY),
                pl.BlockSpec(memory_space=pl.ANY),
            ],
            out_specs=[pl.BlockSpec(memory_space=pltpu.VMEM)] * 3,
            scratch_shapes=[
                pltpu.SMEM(dirichlet.shape, f32),
                pltpu.SMEM(mix_weight.shape, f32),
                pltpu.SMEM(background.shape, f32),
                pltpu.VMEM((high, across), jnp.int32),
                pltpu.VMEM((NZ, LANES, LANES), jnp.int32),
                pltpu.VMEM((NZ, LANES, LANES), jnp.int32),
                pltpu.VMEM((NZ, 16, LANES), f32),
                tile,
                tile,
                pltpu.VMEM((NZ, 16, LANES), f32),
                pltpu.VMEM((ITERS + 1, ny, 16, LANES), f32),
                pltpu.VMEM((ITERS + 1, NZ, 24, LANES), f32),
                pltpu.VMEM((ITERS + 1, cols, 24, LANES), f32),
                pltpu.VMEM((NZ, 16, LANES), f32),
                pltpu.VMEM((LANES, NZ * LANES), f32),
                pltpu.VMEM((48, LANES), bf16),
                pltpu.VMEM((LANES, NZ * LANES), bf16),
                pltpu.VMEM((LANES, NZ * LANES), bf16),
                pltpu.VMEM((16, NZ * LANES), bf16),
                pltpu.VMEM((48, NZ * LANES), bf16),
                pltpu.VMEM((COMPONENTS, 16, LANES), f32),
                tile,
                tile,
                tile,
                tile,
                tile,
                tile,
                tile,
                tile,
                tile,
                pltpu.VMEM((8, LANES), f32),
                pltpu.VMEM((24, LANES), f32),
                pltpu.SemaphoreType.DMA,
                pltpu.SemaphoreType.DMA((3,)),
                pltpu.SemaphoreType.DMA((EXCHANGES, 7)),
                pltpu.SemaphoreType.DMA((EXCHANGES, 7)),
            ],
            compiler_params=pltpu.CompilerParams(collective_id=0, has_side_effects=True),
        )(residues, dirichlet, mix_weight, background)
        return profile, scores.reshape(-1), weights.reshape(-1)

    in_specs = (P("rows", "cols"), P(), P(), P())
    out_specs = (P(None, "cols"), P("rows"), P("rows"))
    return jax.shard_map(body, mesh=mesh, in_specs=in_specs, out_specs=out_specs, check_vma=False)
```

```python
import functools
import math

import jax
import jax.numpy as jnp
from jax import lax
from jax.experimental import pallas as pl
from jax.experimental.pallas import tpu as pltpu
from jax.sharding import PartitionSpec as P

MESH = pl.DeviceIdType.MESH
ALPHABET = 20
PAIRS = 10
COMPONENTS = 9
ITERS = 3
COUNT_MASS = 64.0
NZ = 8
LANES = 128
HALF = 64
Y_ROWS = 11
AT_BG = COMPONENTS * (ALPHABET + 1)
S_ROWS = 17

COUNT_Z, MOVE, GATHER, Y0 = 0, 1, 2, 3
Z0 = Y0 + ITERS + 1
C0 = Z0 + ITERS + 1
EXCHANGES = C0 + ITERS + 1
ORDER = (4, 3, 5, 2, 6, 1, 7)

f32 = jnp.float32
bf16 = jnp.bfloat16


def lgamma(x):
    t = x * (x + 3.0)
    z = x + 4.0
    r = 1.0 / z
    r2 = r * r
    series = r * (1.0 / 12.0 + r2 * (-1.0 / 360.0 + r2 * (1.0 / 1260.0 - r2 * (1.0 / 1680.0))))
    return (z - 0.5) * jnp.log(z) - z + (0.9189385332046727 + series) - jnp.log(t * (t + 2.0))


def iota(shape, dim):
    return lax.broadcasted_iota(jnp.int32, shape, dim)


def low(shape):
    return iota(shape, len(shape) - 1) < HALF


def swap(v):
    return pltpu.roll(v, HALF, 1)


def fold(v):
    return v + swap(v)


def over_rows(v):
    return jnp.sum(v, axis=0, keepdims=True)


def over_lanes(v):
    return jnp.sum(v, axis=1, keepdims=True)


def pick(x, rows):
    bits = [(x & (1 << b)) != 0 for b in range(5)]
    a = [jnp.where(bits[0], rows[2 * i + 1], rows[2 * i]) for i in range(10)]
    b = [jnp.where(bits[1], a[2 * i + 1], a[2 * i]) for i in range(5)]
    c = [jnp.where(bits[2], b[1], b[0]), jnp.where(bits[2], b[3], b[2]), jnp.where(bits[2], rows[20], b[4])]
    return jnp.where(bits[4], c[2], jnp.where(bits[3], c[1], c[0]))


def packed(totals):
    first = low((8, LANES))
    rows = []
    for p in range(PAIRS):
        u, v = totals[p], totals[p + PAIRS]
        rows.append(over_rows(jnp.where(first, u, v) + swap(jnp.where(first, v, u))))
    return rows


def kernel(
    dims,
    res_hbm,
    par_hbm,
    prof_o,
    line_o,
    par_s,
    res_v,
    stage,
    held,
    cnt_send,
    cnt_lo,
    cnt_hi,
    cbuf,
    ybuf,
    zbuf,
    sbuf,
    pbuf,
    wide,
    pieces,
    val_hi,
    val_mid,
    ones1,
    ones3,
    alpha,
    base,
    strength,
    inv_bg,
    lik,
    counts,
    hen,
    inc,
    raw_s,
    score_s,
    mass_s,
    table,
    in_sem,
    small_sem,
    ssem,
    rsem,
):
    ny, nc, seqs, length = dims
    row = lax.axis_index("rows")
    me_c = lax.axis_index("cols")
    me_y, me_z = row // NZ, row % NZ

    def peer(axis, d):
        if axis == "z":
            return (me_y * NZ + (me_z + d) % NZ, me_c)
        if axis == "y":
            return (((me_y + d) % ny) * NZ + me_z, me_c)
        return (row, (me_c + d) % nc)

    size = {"z": NZ, "y": ny, "c": nc}
    mine = {"z": me_z, "y": me_y, "c": me_c}

    barrier = pltpu.get_barrier_semaphore()
    for axis in "yzc":
        for d in range(1, size[axis]):
            pl.semaphore_signal(barrier, inc=1, device_id=peer(axis, d), device_id_type=MESH)
    load = pltpu.make_async_copy(res_hbm, res_v, in_sem)
    load.start()
    small = [pltpu.make_async_copy(par_hbm, par_s, small_sem.at[0])]
    for copy in small:
        copy.start()

    def remote(src, dst, number, axis, d):
        return pltpu.make_async_remote_copy(
            src_ref=src,
            dst_ref=dst,
            send_sem=ssem.at[number, d - 1],
            recv_sem=rsem.at[number, d - 1],
            device_id=peer(axis, d),
            device_id_type=MESH,
        )

    def distances(axis):
        n = size[axis]
        return ORDER if n == 8 else tuple(range(1, n))

    def copies(buf, rows, number, axis):
        me = mine[axis]
        own = buf.at[me, pl.ds(0, rows)]
        return [remote(own, own, number, axis, d) for d in distances(axis)]

    def begin(made):
        for copy in made:
            copy.start()

    def arrive(made):
        for copy in made:
            copy.wait_recv()

    def leave(made):
        for copy in made:
            copy.wait_send()

    def total_of(buf, axis):
        s = buf[0]
        for i in range(1, size[axis]):
            s = s + buf[i]
        return s

    row16 = iota((16, LANES), 0)
    low16 = low((16, LANES))
    load.wait()

    for zd in range(NZ):
        block = pl.ds((zd // 2) * LANES, LANES)
        a, b = res_v[0:LANES, block], res_v[LANES : 2 * LANES, block]
        first = low((LANES, LANES))
        if zd % 2 == 0:
            stage[zd] = jnp.where(first, a, swap(b))
        else:
            stage[zd] = jnp.where(first, swap(a), b)

    def count_one(zd, carry):
        fields = [jnp.zeros((8, LANES), jnp.int32) for _ in range(5)]
        for t in range(LANES // 8):
            x = stage[zd, t * 8 : t * 8 + 8, :]
            unit = jnp.left_shift(jnp.ones((8, LANES), jnp.int32), (x & 3) * 8)
            which = x >> 2
            fields = [fields[q] + jnp.where(which == q, unit, 0) for q in range(5)]
        for q in range(5):
            v = fields[q]
            for step in (4, 2, 1):
                v = v + pltpu.roll(v, step, 0)
            for r in range(4):
                p = 4 * q + r
                line = ((v >> (8 * r)) & 255).astype(f32)
                if p < PAIRS:
                    cnt_lo[p : p + 1, :] = line[0:1]
                else:
                    cnt_hi[p - PAIRS : p - PAIRS + 1, :] = line[0:1]
        u, v = cnt_lo[...], cnt_hi[...]
        cnt_send[zd] = jnp.where(low16, u, v) + swap(jnp.where(low16, v, u))
        return carry

    lax.fori_loop(0, NZ, count_one, 0)
    cbuf[me_z] = cnt_send[me_z]
    held[me_z] = stage[me_z]

    pl.semaphore_wait(barrier, ny + NZ + nc - 3)

    sent_counts = []
    for d in distances("z"):
        other = (me_z + d) % NZ
        sent_counts.append(
            remote(cnt_send.at[other, pl.ds(0, PAIRS)], cbuf.at[me_z, pl.ds(0, PAIRS)], COUNT_Z, "z", d)
        )
    moved = [remote(stage.at[(me_z + d) % NZ], held.at[me_z], MOVE, "z", d) for d in distances("z")]
    begin(sent_counts)
    begin(moved)

    for b in range(NZ):
        half = (iota((16, LANES), 1) >= HALF).astype(jnp.int32)
        spread = jnp.where(row16 == 2 * b + half, 1.0, 0.0).astype(bf16)
        ones1[:, b * LANES : (b + 1) * LANES] = spread
        for n in range(3):
            ones3[16 * n : 16 * n + 16, b * LANES : (b + 1) * LANES] = spread
    low1 = low((1, LANES))
    for copy in small:
        copy.wait()
    for k in range(COMPONENTS):
        alpha[k] = jnp.ones((16, LANES), f32)
        for p in range(PAIRS):
            alpha[k, p : p + 1, :] = jnp.where(low1, par_s[k * ALPHABET + p], par_s[k * ALPHABET + p + PAIRS])
    inv_bg[...] = jnp.ones((16, LANES), f32)
    for p in range(PAIRS):
        inv_bg[p : p + 1, :] = jnp.where(low1, par_s[AT_BG + p], par_s[AT_BG + p + PAIRS])
    bg = inv_bg[...]
    inv_bg[...] = jnp.where(row16 < PAIRS, over_rows(fold(jnp.where(row16 < PAIRS, bg, 0.0))) / bg, 1.0)
    strength[...] = jnp.ones((16, LANES), f32)
    base[...] = jnp.zeros((16, LANES), f32)
    lik[...] = jnp.ones((16, LANES), f32)
    for k in range(COMPONENTS):
        al = alpha[k]
        strength[k : k + 1, :] = over_rows(fold(jnp.where(row16 < PAIRS, al, 0.0)))
        base[k : k + 1, :] = over_rows(fold(lgamma(al)))
        lik[k : k + 1, :] = jnp.where(low1, par_s[COMPONENTS * ALPHABET + k], par_s[COMPONENTS * ALPHABET + k])
    mix = lik[...]
    log_prior = jnp.log(mix) - jnp.log(over_rows(jnp.where(row16 < COMPONENTS, mix, 0.0)))
    base[...] = log_prior + lgamma(strength[...]) - base[...]

    arrive(sent_counts)
    ybuf[0, me_y] = total_of(cbuf, "z")
    ex = copies(ybuf.at[0], Y_ROWS, Y0, "y")
    begin(ex)
    arrive(ex)
    number = jnp.where(row16 < PAIRS, total_of(ybuf.at[0], "y"), 0.0)
    counts[...] = number
    gap = seqs - over_rows(fold(number))
    present = number > 0.5
    distinct = over_rows(fold(jnp.where(present, 1.0, 0.0))) + jnp.where(gap > 0.5, 1.0, 0.0)
    inverse = jnp.where(present, 1.0 / (distinct * jnp.maximum(number, 1.0)), 0.0)
    gap_inverse = jnp.where(gap > 0.5, 1.0 / (distinct * jnp.maximum(gap, 1.0)), 0.0)

    def set_table(lines, gap_line):
        other = swap(lines)
        table[0:PAIRS, :] = jnp.where(low16, lines, other)[0:PAIRS]
        table[PAIRS:ALPHABET, :] = jnp.where(low16, other, lines)[0:PAIRS]
        table[ALPHABET : ALPHABET + 1, :] = gap_line

    def sums_of_table(arriving=None):
        rows = [jnp.broadcast_to(table[a : a + 1, :], (16, LANES)) for a in range(ALPHABET + 1)]

        def look_up(b, at):
            v = pick(held[b, pl.ds(at, 16), :], rows)
            hi = v.astype(bf16)
            columns = pl.ds(b * LANES if isinstance(b, int) else pl.multiple_of(b * LANES, LANES), LANES)
            val_hi[pl.ds(at, 16), columns] = hi
            val_mid[pl.ds(at, 16), columns] = (v - hi.astype(f32)).astype(bf16)

        if arriving is None:

            def group(g, carry):
                for b in range(NZ):
                    look_up(b, pl.multiple_of(g * 16, 16))
                return carry

            lax.fori_loop(0, LANES // 16, group, 0)
        else:
            for b, copy in arriving:
                if copy is not None:
                    copy.wait_recv()

                def group(g, carry):
                    for u in range(4):
                        look_up(b, pl.multiple_of(g * 64 + u * 16, 16))
                    return carry

                lax.fori_loop(0, LANES // 64, group, 0)
        nt = (((1,), (1,)), ((), ()))
        e = ones1[...]
        return lax.dot_general(e, val_hi[...], nt, preferred_element_type=f32) + lax.dot_general(
            e, val_mid[...], nt, preferred_element_type=f32
        )

    def sum_over_columns(i, part, extra):
        zbuf[i, me_z, 0:16, :] = part
        zbuf[i, me_z, 16:24, :] = extra
        ex = copies(zbuf.at[i], S_ROWS, Z0 + i, "z")
        begin(ex)
        arrive(ex)
        sbuf[i, me_c] = total_of(zbuf.at[i], "z")
        ex = copies(sbuf.at[i], S_ROWS, C0 + i, "c")
        begin(ex)
        arrive(ex)
        return total_of(sbuf.at[i], "c")

    set_table(inverse, gap_inverse)
    arriving = [(me_z, None)]
    for d, copy in zip(distances("z"), moved):
        arriving.append(((me_z + NZ - d) % NZ, copy))
    hen[...] = sum_over_columns(0, sums_of_table(arriving), jnp.zeros((8, LANES), f32))[0:16] * (1.0 / length)
    inc[...] = jnp.ones((16, LANES), f32)

    def weighted_counts(i):
        def group(g, totals):
            for b in range(NZ):
                at = pl.multiple_of(g * 8, 8)
                x = held[b, pl.ds(at, 8), :]
                w = wide[pl.ds(at, 8), b * LANES : (b + 1) * LANES]
                totals = tuple(totals[a] + jnp.where(x == a, w, 0.0) for a in range(ALPHABET))
            return totals

        totals = lax.fori_loop(0, LANES // 8, group, tuple(jnp.zeros((8, LANES), f32) for _ in range(ALPHABET)))
        for p, line in enumerate(packed(totals)):
            ybuf[i, me_y, p : p + 1, :] = line

    def mixture(frequency):
        column_total = over_rows(fold(frequency))
        for k in range(COMPONENTS):
            lik[k : k + 1, :] = over_rows(lgamma(frequency + alpha[k]))
        lam = fold(lik[...]) + base[...] - lgamma(strength[...] + column_total)
        lam = jnp.where(row16 < COMPONENTS, lam, -1e30)
        e = jnp.exp(lam - jnp.max(lam, axis=0, keepdims=True))
        shares = e / (over_rows(e) * (column_total + strength[...]))
        smoothed = jnp.zeros((16, LANES), f32)
        for k in range(COMPONENTS):
            smoothed = smoothed + shares[k : k + 1, :] * (frequency + alpha[k])
        return jnp.log(smoothed * inv_bg[...])

    gathered = copies(pbuf, PAIRS, GATHER, "z")

    def iteration(it, carry):
        i = it + 1
        raw = hen[...] * inc[...]
        raw_s[...] = raw
        part_mass = jnp.broadcast_to(over_lanes(over_rows(raw)), (1, LANES))
        hi = raw.astype(bf16)
        rest = raw - hi.astype(f32)
        mid = rest.astype(bf16)
        pieces[0:16, :] = hi
        pieces[16:32, :] = mid
        pieces[32:48, :] = (rest - mid.astype(f32)).astype(bf16)
        wide[...] = lax.dot_general(
            pieces[...], ones3[...], (((0,), (0,)), ((), ())), preferred_element_type=f32
        )
        weighted_counts(i)
        ybuf[i, me_y, PAIRS : PAIRS + 1, :] = part_mass
        ex = copies(ybuf.at[i], Y_ROWS, Y0 + i, "y")
        begin(ex)
        arrive(ex)
        whole = total_of(ybuf.at[i], "y")
        mass = whole[PAIRS : PAIRS + 1, :]
        mass_s[...] = jnp.broadcast_to(mass, (8, LANES))
        frequency = jnp.where(row16 < PAIRS, whole, 0.0) * (COUNT_MASS / mass)
        profile = mixture(frequency)

        @pl.when(it == ITERS - 1)
        def _():
            pbuf[me_z] = profile
            begin(gathered)

        set_table(profile, jnp.zeros((1, LANES), f32))
        share = over_lanes(over_rows(jnp.where(row16 < PAIRS, profile * counts[...], 0.0)))
        extra = jnp.where(iota((8, LANES), 0) == 0, share, 0.0)
        done = sum_over_columns(i, sums_of_table(), extra)
        scores = done[0:16] * (1.0 / length)
        center = done[16:17, :] * (1.0 / (length * seqs))
        score_s[...] = scores
        inc[...] = 1.0 / (1.0 + jnp.exp((center - scores) * math.sqrt(length)))
        return carry

    lax.fori_loop(0, ITERS, iteration, 0)

    weights = raw_s[...] * (seqs / mass_s[0:1, :])
    scores = score_s[...]
    own_w, own_s = weights[0:2], scores[0:2]
    for b in range(1, NZ):
        own_w = jnp.where(me_z == b, weights[2 * b : 2 * b + 2], own_w)
        own_s = jnp.where(me_z == b, scores[2 * b : 2 * b + 2], own_s)
    line_o[0:2, :] = own_s
    line_o[2:4, :] = own_w

    arrive(gathered)
    for block in range(NZ // 2):
        even, odd = pbuf[2 * block], pbuf[2 * block + 1]
        at = pl.ds(block * LANES, LANES)
        prof_o[0:PAIRS, at] = jnp.where(low16, even, swap(odd))[0:PAIRS]
        prof_o[PAIRS:ALPHABET, at] = jnp.where(low16, swap(even), odd)[0:PAIRS]

    leave(sent_counts)
    leave(moved)
    leave(gathered)
    for i in range(ITERS + 1):
        leave(copies(ybuf.at[i], Y_ROWS, Y0 + i, "y"))
        leave(copies(zbuf.at[i], S_ROWS, Z0 + i, "z"))
        leave(copies(sbuf.at[i], S_ROWS, C0 + i, "c"))


def solution(mesh):
    rows, cols = mesh.shape["rows"], mesh.shape["cols"]
    ny = rows // NZ

    def body(residues, dirichlet, mix_weight, background):
        high, across = residues.shape
        dims = (ny, cols, high * rows, across * cols)
        tile = pltpu.VMEM((16, LANES), f32)
        small = jnp.concatenate([dirichlet.reshape(-1), mix_weight, background])
        small = jnp.pad(small, (0, 256 - small.shape[0]))
        profile, lines = pl.pallas_call(
            functools.partial(kernel, dims),
            out_shape=(
                jax.ShapeDtypeStruct((ALPHABET, across), f32),
                jax.ShapeDtypeStruct((4, LANES), f32),
            ),
            in_specs=[
                pl.BlockSpec(memory_space=pl.ANY),
                pl.BlockSpec(memory_space=pl.ANY),
            ],
            out_specs=[pl.BlockSpec(memory_space=pltpu.VMEM)] * 2,
            scratch_shapes=[
                pltpu.SMEM((256,), f32),
                pltpu.VMEM((high, across), jnp.int32),
                pltpu.VMEM((NZ, LANES, LANES), jnp.int32),
                pltpu.VMEM((NZ, LANES, LANES), jnp.int32),
                pltpu.VMEM((NZ, 16, LANES), f32),
                tile,
                tile,
                pltpu.VMEM((NZ, 16, LANES), f32),
                pltpu.VMEM((ITERS + 1, ny, 16, LANES), f32),
                pltpu.VMEM((ITERS + 1, NZ, 24, LANES), f32),
                pltpu.VMEM((ITERS + 1, cols, 24, LANES), f32),
                pltpu.VMEM((NZ, 16, LANES), f32),
                pltpu.VMEM((LANES, NZ * LANES), f32),
                pltpu.VMEM((48, LANES), bf16),
                pltpu.VMEM((LANES, NZ * LANES), bf16),
                pltpu.VMEM((LANES, NZ * LANES), bf16),
                pltpu.VMEM((16, NZ * LANES), bf16),
                pltpu.VMEM((48, NZ * LANES), bf16),
                pltpu.VMEM((COMPONENTS, 16, LANES), f32),
                tile,
                tile,
                tile,
                tile,
                tile,
                tile,
                tile,
                tile,
                tile,
                pltpu.VMEM((8, LANES), f32),
                pltpu.VMEM((24, LANES), f32),
                pltpu.SemaphoreType.DMA,
                pltpu.SemaphoreType.DMA((3,)),
                pltpu.SemaphoreType.DMA((EXCHANGES, 7)),
                pltpu.SemaphoreType.DMA((EXCHANGES, 7)),
            ],
            compiler_params=pltpu.CompilerParams(
                collective_id=0, has_side_effects=True, vmem_limit_bytes=56_500_000
            ),
        )(residues, small)
        return profile, lines[0:2].reshape(-1), lines[2:4].reshape(-1)

    in_specs = (P("rows", "cols"), P(), P(), P())
    out_specs = (P(None, "cols"), P("rows"), P("rows"))
    return jax.shard_map(body, mesh=mesh, in_specs=in_specs, out_specs=out_specs, check_vma=False)
```

```python
import functools
import math

import jax
import jax.numpy as jnp
from jax import lax
from jax.experimental import pallas as pl
from jax.experimental.pallas import tpu as pltpu
from jax.sharding import PartitionSpec as P

MESH = pl.DeviceIdType.MESH
ALPHABET = 20
PAIRS = 10
COMPONENTS = 9
ITERS = 3
COUNT_MASS = 64.0
NZ = 8
LANES = 128
HALF = 64
Y_ROWS = 11
AT_BG = COMPONENTS * (ALPHABET + 1)
S_ROWS = 17

COUNT_Z, MOVE, GATHER, Y0 = 0, 1, 2, 3
Z0 = Y0 + ITERS + 1
C0 = Z0 + ITERS + 1
EXCHANGES = C0 + ITERS + 1
ORDER = (4, 3, 5, 2, 6, 1, 7)

f32 = jnp.float32
bf16 = jnp.bfloat16


def lgamma(x):
    t = x * (x + 3.0)
    z = x + 4.0
    r = 1.0 / z
    r2 = r * r
    series = r * (1.0 / 12.0 + r2 * (-1.0 / 360.0 + r2 * (1.0 / 1260.0 - r2 * (1.0 / 1680.0))))
    return (z - 0.5) * jnp.log(z) - z + (0.9189385332046727 + series) - jnp.log(t * (t + 2.0))


def iota(shape, dim):
    return lax.broadcasted_iota(jnp.int32, shape, dim)


def low(shape):
    return iota(shape, len(shape) - 1) < HALF


def swap(v):
    return pltpu.roll(v, HALF, 1)


def fold(v):
    return v + swap(v)


def over_rows(v):
    return jnp.sum(v, axis=0, keepdims=True)


def over_lanes(v):
    return jnp.sum(v, axis=1, keepdims=True)


def pick(x, rows):
    bits = [(x & (1 << b)) != 0 for b in range(5)]
    a = [jnp.where(bits[0], rows[2 * i + 1], rows[2 * i]) for i in range(10)]
    b = [jnp.where(bits[1], a[2 * i + 1], a[2 * i]) for i in range(5)]
    c = [jnp.where(bits[2], b[1], b[0]), jnp.where(bits[2], b[3], b[2]), jnp.where(bits[2], rows[20], b[4])]
    return jnp.where(bits[4], c[2], jnp.where(bits[3], c[1], c[0]))


def packed(totals):
    first = low((8, LANES))
    rows = []
    for p in range(PAIRS):
        u, v = totals[p], totals[p + PAIRS]
        rows.append(over_rows(jnp.where(first, u, v) + swap(jnp.where(first, v, u))))
    return rows


def kernel(
    dims,
    res_hbm,
    par_hbm,
    prof_o,
    line_o,
    par_s,
    res_v,
    stage,
    held,
    cnt_send,
    cnt_lo,
    cnt_hi,
    cbuf,
    ybuf,
    zbuf,
    sbuf,
    pbuf,
    wide,
    pieces,
    val_hi,
    val_mid,
    ones1,
    ones3,
    alpha,
    base,
    strength,
    inv_bg,
    lik,
    counts,
    hen,
    inc,
    raw_s,
    score_s,
    mass_s,
    table,
    in_sem,
    small_sem,
    ssem,
    rsem,
):
    ny, nc, seqs, length = dims
    row = lax.axis_index("rows")
    me_c = lax.axis_index("cols")
    me_y, me_z = row // NZ, row % NZ

    def peer(axis, d):
        if axis == "z":
            return (me_y * NZ + (me_z + d) % NZ, me_c)
        if axis == "y":
            return (((me_y + d) % ny) * NZ + me_z, me_c)
        return (row, (me_c + d) % nc)

    size = {"z": NZ, "y": ny, "c": nc}
    mine = {"z": me_z, "y": me_y, "c": me_c}

    barrier = pltpu.get_barrier_semaphore()
    for axis in "yzc":
        for d in range(1, size[axis]):
            pl.semaphore_signal(barrier, inc=1, device_id=peer(axis, d), device_id_type=MESH)
    load = pltpu.make_async_copy(res_hbm, res_v, in_sem)
    load.start()
    small = [pltpu.make_async_copy(par_hbm, par_s, small_sem.at[0])]
    for copy in small:
        copy.start()

    def remote(src, dst, number, axis, d):
        return pltpu.make_async_remote_copy(
            src_ref=src,
            dst_ref=dst,
            send_sem=ssem.at[number, d - 1],
            recv_sem=rsem.at[number, d - 1],
            device_id=peer(axis, d),
            device_id_type=MESH,
        )

    def distances(axis):
        n = size[axis]
        return ORDER if n == 8 else tuple(range(1, n))

    def copies(buf, rows, number, axis):
        me = mine[axis]
        own = buf.at[me, pl.ds(0, rows)]
        return [remote(own, own, number, axis, d) for d in distances(axis)]

    def begin(made):
        for copy in made:
            copy.start()

    def arrive(made):
        for copy in made:
            copy.wait_recv()

    def leave(made):
        for copy in made:
            copy.wait_send()

    def total_of(buf, axis):
        s = buf[0]
        for i in range(1, size[axis]):
            s = s + buf[i]
        return s

    row16 = iota((16, LANES), 0)
    low16 = low((16, LANES))
    load.wait()

    for zd in range(NZ):
        block = pl.ds((zd // 2) * LANES, LANES)
        a, b = res_v[0:LANES, block], res_v[LANES : 2 * LANES, block]
        first = low((LANES, LANES))
        if zd % 2 == 0:
            stage[zd] = jnp.where(first, a, swap(b))
        else:
            stage[zd] = jnp.where(first, swap(a), b)

    def count_one(zd, carry):
        fields = [jnp.zeros((8, LANES), jnp.int32) for _ in range(5)]
        for t in range(LANES // 8):
            x = stage[zd, t * 8 : t * 8 + 8, :]
            unit = jnp.left_shift(jnp.ones((8, LANES), jnp.int32), (x & 3) * 8)
            which = x >> 2
            fields = [fields[q] + jnp.where(which == q, unit, 0) for q in range(5)]
        for q in range(5):
            v = fields[q]
            for step in (4, 2, 1):
                v = v + pltpu.roll(v, step, 0)
            for r in range(4):
                p = 4 * q + r
                line = ((v >> (8 * r)) & 255).astype(f32)
                if p < PAIRS:
                    cnt_lo[p : p + 1, :] = line[0:1]
                else:
                    cnt_hi[p - PAIRS : p - PAIRS + 1, :] = line[0:1]
        u, v = cnt_lo[...], cnt_hi[...]
        cnt_send[zd] = jnp.where(low16, u, v) + swap(jnp.where(low16, v, u))
        return carry

    lax.fori_loop(0, NZ, count_one, 0)
    cbuf[me_z] = cnt_send[me_z]
    held[me_z] = stage[me_z]

    pl.semaphore_wait(barrier, ny + NZ + nc - 3)

    sent_counts = []
    for d in distances("z"):
        other = (me_z + d) % NZ
        sent_counts.append(
            remote(cnt_send.at[other, pl.ds(0, PAIRS)], cbuf.at[me_z, pl.ds(0, PAIRS)], COUNT_Z, "z", d)
        )
    moved = [remote(stage.at[(me_z + d) % NZ], held.at[me_z], MOVE, "z", d) for d in distances("z")]
    begin(sent_counts)
    begin(moved)

    for b in range(NZ):
        half = (iota((16, LANES), 1) >= HALF).astype(jnp.int32)
        spread = jnp.where(row16 == 2 * b + half, 1.0, 0.0).astype(bf16)
        ones1[:, b * LANES : (b + 1) * LANES] = spread
        for n in range(3):
            ones3[16 * n : 16 * n + 16, b * LANES : (b + 1) * LANES] = spread
    low1 = low((1, LANES))
    for copy in small:
        copy.wait()
    for k in range(COMPONENTS):
        alpha[k] = jnp.ones((16, LANES), f32)
        for p in range(PAIRS):
            alpha[k, p : p + 1, :] = jnp.where(low1, par_s[k * ALPHABET + p], par_s[k * ALPHABET + p + PAIRS])
    inv_bg[...] = jnp.ones((16, LANES), f32)
    for p in range(PAIRS):
        inv_bg[p : p + 1, :] = jnp.where(low1, par_s[AT_BG + p], par_s[AT_BG + p + PAIRS])
    bg = inv_bg[...]
    inv_bg[...] = jnp.where(row16 < PAIRS, over_rows(fold(jnp.where(row16 < PAIRS, bg, 0.0))) / bg, 1.0)
    strength[...] = jnp.ones((16, LANES), f32)
    base[...] = jnp.zeros((16, LANES), f32)
    lik[...] = jnp.ones((16, LANES), f32)
    for k in range(COMPONENTS):
        al = alpha[k]
        strength[k : k + 1, :] = over_rows(fold(jnp.where(row16 < PAIRS, al, 0.0)))
        base[k : k + 1, :] = over_rows(fold(lgamma(al)))
        lik[k : k + 1, :] = jnp.where(low1, par_s[COMPONENTS * ALPHABET + k], par_s[COMPONENTS * ALPHABET + k])
    mix = lik[...]
    log_prior = jnp.log(mix) - jnp.log(over_rows(jnp.where(row16 < COMPONENTS, mix, 0.0)))
    base[...] = log_prior + lgamma(strength[...]) - base[...]

    arrive(sent_counts)
    ybuf[0, me_y] = total_of(cbuf, "z")
    ex = copies(ybuf.at[0], Y_ROWS, Y0, "y")
    begin(ex)
    arrive(ex)
    number = jnp.where(row16 < PAIRS, total_of(ybuf.at[0], "y"), 0.0)
    counts[...] = number
    gap = seqs - over_rows(fold(number))
    present = number > 0.5
    distinct = over_rows(fold(jnp.where(present, 1.0, 0.0))) + jnp.where(gap > 0.5, 1.0, 0.0)
    inverse = jnp.where(present, 1.0 / (distinct * jnp.maximum(number, 1.0)), 0.0)
    gap_inverse = jnp.where(gap > 0.5, 1.0 / (distinct * jnp.maximum(gap, 1.0)), 0.0)

    def set_table(lines, gap_line):
        other = swap(lines)
        table[0:PAIRS, :] = jnp.where(low16, lines, other)[0:PAIRS]
        table[PAIRS:ALPHABET, :] = jnp.where(low16, other, lines)[0:PAIRS]
        table[ALPHABET : ALPHABET + 1, :] = gap_line

    def sums_of_table(arriving=None):
        rows = [jnp.broadcast_to(table[a : a + 1, :], (16, LANES)) for a in range(ALPHABET + 1)]

        def look_up(b, at):
            v = pick(held[b, pl.ds(at, 16), :], rows)
            hi = v.astype(bf16)
            columns = pl.ds(b * LANES if isinstance(b, int) else pl.multiple_of(b * LANES, LANES), LANES)
            val_hi[pl.ds(at, 16), columns] = hi
            val_mid[pl.ds(at, 16), columns] = (v - hi.astype(f32)).astype(bf16)

        if arriving is None:

            def group(g, carry):
                for b in range(NZ):
                    look_up(b, pl.multiple_of(g * 16, 16))
                return carry

            lax.fori_loop(0, LANES // 16, group, 0)
        else:
            for b, copy in arriving:
                if copy is not None:
                    copy.wait_recv()

                def group(g, carry):
                    for u in range(4):
                        look_up(b, pl.multiple_of(g * 64 + u * 16, 16))
                    return carry

                lax.fori_loop(0, LANES // 64, group, 0)
        nt = (((1,), (1,)), ((), ()))
        e = ones1[...]
        return lax.dot_general(e, val_hi[...], nt, preferred_element_type=f32) + lax.dot_general(
            e, val_mid[...], nt, preferred_element_type=f32
        )

    def sum_over_columns(i, part, extra, meanwhile=None):
        zbuf[i, me_z, 0:16, :] = part
        zbuf[i, me_z, 16:24, :] = extra
        ex = copies(zbuf.at[i], S_ROWS, Z0 + i, "z")
        begin(ex)
        arrive(ex)
        sbuf[i, me_c] = total_of(zbuf.at[i], "z")
        ex = copies(sbuf.at[i], S_ROWS, C0 + i, "c")
        begin(ex)
        if meanwhile is not None:
            meanwhile()
        arrive(ex)
        return total_of(sbuf.at[i], "c")

    set_table(inverse, gap_inverse)
    arriving = [(me_z, None)]
    for d, copy in zip(distances("z"), moved):
        arriving.append(((me_z + NZ - d) % NZ, copy))
    hen[...] = sum_over_columns(0, sums_of_table(arriving), jnp.zeros((8, LANES), f32))[0:16] * (1.0 / length)
    inc[...] = jnp.ones((16, LANES), f32)

    def weighted_counts(i):
        def group(g, totals):
            for b in range(NZ):
                at = pl.multiple_of(g * 8, 8)
                x = held[b, pl.ds(at, 8), :]
                w = wide[pl.ds(at, 8), b * LANES : (b + 1) * LANES]
                totals = tuple(totals[a] + jnp.where(x == a, w, 0.0) for a in range(ALPHABET))
            return totals

        totals = lax.fori_loop(0, LANES // 8, group, tuple(jnp.zeros((8, LANES), f32) for _ in range(ALPHABET)))
        for p, line in enumerate(packed(totals)):
            ybuf[i, me_y, p : p + 1, :] = line

    def mixture(frequency):
        column_total = over_rows(fold(frequency))
        for k in range(COMPONENTS):
            lik[k : k + 1, :] = over_rows(lgamma(frequency + alpha[k]))
        lam = fold(lik[...]) + base[...] - lgamma(strength[...] + column_total)
        lam = jnp.where(row16 < COMPONENTS, lam, -1e30)
        e = jnp.exp(lam - jnp.max(lam, axis=0, keepdims=True))
        shares = e / (over_rows(e) * (column_total + strength[...]))
        smoothed = jnp.zeros((16, LANES), f32)
        for k in range(COMPONENTS):
            smoothed = smoothed + shares[k : k + 1, :] * (frequency + alpha[k])
        return jnp.log(smoothed * inv_bg[...])

    gathered = copies(pbuf, PAIRS, GATHER, "z")

    def finish_profile():
        arrive(gathered)
        for block in range(NZ // 2):
            even, odd = pbuf[2 * block], pbuf[2 * block + 1]
            at = pl.ds(block * LANES, LANES)
            prof_o[0:PAIRS, at] = jnp.where(low16, even, swap(odd))[0:PAIRS]
            prof_o[PAIRS:ALPHABET, at] = jnp.where(low16, swap(even), odd)[0:PAIRS]
        leave(sent_counts)
        leave(moved)
        leave(gathered)
        for i in range(ITERS + 1):
            leave(copies(ybuf.at[i], Y_ROWS, Y0 + i, "y"))
            leave(copies(zbuf.at[i], S_ROWS, Z0 + i, "z"))
            if i < ITERS:
                leave(copies(sbuf.at[i], S_ROWS, C0 + i, "c"))

    def iteration(it, carry):
        i = it + 1
        raw = hen[...] * inc[...]
        raw_s[...] = raw
        part_mass = jnp.broadcast_to(over_lanes(over_rows(raw)), (1, LANES))
        hi = raw.astype(bf16)
        rest = raw - hi.astype(f32)
        mid = rest.astype(bf16)
        pieces[0:16, :] = hi
        pieces[16:32, :] = mid
        pieces[32:48, :] = (rest - mid.astype(f32)).astype(bf16)
        wide[...] = lax.dot_general(
            pieces[...], ones3[...], (((0,), (0,)), ((), ())), preferred_element_type=f32
        )
        weighted_counts(i)
        ybuf[i, me_y, PAIRS : PAIRS + 1, :] = part_mass
        ex = copies(ybuf.at[i], Y_ROWS, Y0 + i, "y")
        begin(ex)
        arrive(ex)
        whole = total_of(ybuf.at[i], "y")
        mass = whole[PAIRS : PAIRS + 1, :]
        mass_s[...] = jnp.broadcast_to(mass, (8, LANES))
        frequency = jnp.where(row16 < PAIRS, whole, 0.0) * (COUNT_MASS / mass)
        profile = mixture(frequency)

        @pl.when(it == ITERS - 1)
        def _():
            pbuf[me_z] = profile
            begin(gathered)

        set_table(profile, jnp.zeros((1, LANES), f32))
        share = over_lanes(over_rows(jnp.where(row16 < PAIRS, profile * counts[...], 0.0)))
        extra = jnp.where(iota((8, LANES), 0) == 0, share, 0.0)
        done = sum_over_columns(i, sums_of_table(), extra, lambda: pl.when(it == ITERS - 1)(finish_profile))
        scores = done[0:16] * (1.0 / length)
        center = done[16:17, :] * (1.0 / (length * seqs))
        score_s[...] = scores
        inc[...] = 1.0 / (1.0 + jnp.exp((center - scores) * math.sqrt(length)))
        return carry

    lax.fori_loop(0, ITERS, iteration, 0)

    weights = raw_s[...] * (seqs / mass_s[0:1, :])
    scores = score_s[...]
    own_w, own_s = weights[0:2], scores[0:2]
    for b in range(1, NZ):
        own_w = jnp.where(me_z == b, weights[2 * b : 2 * b + 2], own_w)
        own_s = jnp.where(me_z == b, scores[2 * b : 2 * b + 2], own_s)
    line_o[0:2, :] = own_s
    line_o[2:4, :] = own_w

    leave(copies(sbuf.at[ITERS], S_ROWS, C0 + ITERS, "c"))


def solution(mesh):
    rows, cols = mesh.shape["rows"], mesh.shape["cols"]
    ny = rows // NZ

    def body(residues, dirichlet, mix_weight, background):
        high, across = residues.shape
        dims = (ny, cols, high * rows, across * cols)
        tile = pltpu.VMEM((16, LANES), f32)
        small = jnp.concatenate([dirichlet.reshape(-1), mix_weight, background])
        small = jnp.pad(small, (0, 256 - small.shape[0]))
        profile, lines = pl.pallas_call(
            functools.partial(kernel, dims),
            out_shape=(
                jax.ShapeDtypeStruct((ALPHABET, across), f32),
                jax.ShapeDtypeStruct((4, LANES), f32),
            ),
            in_specs=[
                pl.BlockSpec(memory_space=pl.ANY),
                pl.BlockSpec(memory_space=pl.ANY),
            ],
            out_specs=[pl.BlockSpec(memory_space=pltpu.VMEM)] * 2,
            scratch_shapes=[
                pltpu.SMEM((256,), f32),
                pltpu.VMEM((high, across), jnp.int32),
                pltpu.VMEM((NZ, LANES, LANES), jnp.int32),
                pltpu.VMEM((NZ, LANES, LANES), jnp.int32),
                pltpu.VMEM((NZ, 16, LANES), f32),
                tile,
                tile,
                pltpu.VMEM((NZ, 16, LANES), f32),
                pltpu.VMEM((ITERS + 1, ny, 16, LANES), f32),
                pltpu.VMEM((ITERS + 1, NZ, 24, LANES), f32),
                pltpu.VMEM((ITERS + 1, cols, 24, LANES), f32),
                pltpu.VMEM((NZ, 16, LANES), f32),
                pltpu.VMEM((LANES, NZ * LANES), f32),
                pltpu.VMEM((48, LANES), bf16),
                pltpu.VMEM((LANES, NZ * LANES), bf16),
                pltpu.VMEM((LANES, NZ * LANES), bf16),
                pltpu.VMEM((16, NZ * LANES), bf16),
                pltpu.VMEM((48, NZ * LANES), bf16),
                pltpu.VMEM((COMPONENTS, 16, LANES), f32),
                tile,
                tile,
                tile,
                tile,
                tile,
                tile,
                tile,
                tile,
                tile,
                pltpu.VMEM((8, LANES), f32),
                pltpu.VMEM((24, LANES), f32),
                pltpu.SemaphoreType.DMA,
                pltpu.SemaphoreType.DMA((3,)),
                pltpu.SemaphoreType.DMA((EXCHANGES, 7)),
                pltpu.SemaphoreType.DMA((EXCHANGES, 7)),
            ],
            compiler_params=pltpu.CompilerParams(
                collective_id=0, has_side_effects=True, vmem_limit_bytes=56_500_000
            ),
        )(residues, small)
        return profile, lines[0:2].reshape(-1), lines[2:4].reshape(-1)

    in_specs = (P("rows", "cols"), P(), P(), P())
    out_specs = (P(None, "cols"), P("rows"), P("rows"))
    return jax.shard_map(body, mesh=mesh, in_specs=in_specs, out_specs=out_specs, check_vma=False)
```

```python
import functools
import math

import jax
import jax.numpy as jnp
from jax import lax
from jax.experimental import pallas as pl
from jax.experimental.pallas import tpu as pltpu
from jax.sharding import PartitionSpec as P

MESH = pl.DeviceIdType.MESH
ALPHABET = 20
PAIRS = 10
COMPONENTS = 9
ITERS = 3
COUNT_MASS = 64.0
NZ = 8
LANES = 128
HALF = 64
Y_ROWS = 11
AT_BG = COMPONENTS * (ALPHABET + 1)
S_ROWS = 17

COUNT_Z, MOVE, GATHER, Y0 = 0, 1, 2, 3
Z0 = Y0 + ITERS + 1
C0 = Z0 + ITERS + 1
EXCHANGES = C0 + ITERS + 1
ORDER = (4, 3, 5, 2, 6, 1, 7)

f32 = jnp.float32
bf16 = jnp.bfloat16


def lgamma(x):
    t = x * (x + 3.0)
    z = x + 4.0
    r = 1.0 / z
    r2 = r * r
    series = r * (1.0 / 12.0 + r2 * (-1.0 / 360.0 + r2 * (1.0 / 1260.0 - r2 * (1.0 / 1680.0))))
    return (z - 0.5) * jnp.log(z) - z + (0.9189385332046727 + series) - jnp.log(t * (t + 2.0))


def iota(shape, dim):
    return lax.broadcasted_iota(jnp.int32, shape, dim)


def low(shape):
    return iota(shape, len(shape) - 1) < HALF


def swap(v):
    return pltpu.roll(v, HALF, 1)


def fold(v):
    return v + swap(v)


def over_rows(v):
    return jnp.sum(v, axis=0, keepdims=True)


def over_lanes(v):
    return jnp.sum(v, axis=1, keepdims=True)


def pick(x, rows):
    bits = [(x & (1 << b)) != 0 for b in range(3)] + [x > 7, x > 15]
    a = [jnp.where(bits[0], rows[2 * i + 1], rows[2 * i]) for i in range(10)]
    b = [jnp.where(bits[1], a[2 * i + 1], a[2 * i]) for i in range(5)]
    c = [jnp.where(bits[2], b[1], b[0]), jnp.where(bits[2], b[3], b[2]), jnp.where(bits[2], rows[20], b[4])]
    return jnp.where(bits[4], c[2], jnp.where(bits[3], c[1], c[0]))


def packed(totals):
    first = low((8, LANES))
    rows = []
    for p in range(PAIRS):
        u, v = totals[p], totals[p + PAIRS]
        rows.append(over_rows(jnp.where(first, u, v) + swap(jnp.where(first, v, u))))
    return rows


def kernel(
    dims,
    res_hbm,
    par_hbm,
    prof_o,
    line_o,
    par_s,
    res_v,
    stage,
    held,
    cnt_send,
    cnt_lo,
    cnt_hi,
    cbuf,
    ybuf,
    zbuf,
    sbuf,
    pbuf,
    wide,
    pieces,
    val_hi,
    val_mid,
    ones1,
    ones3,
    alpha,
    base,
    strength,
    inv_bg,
    lik,
    counts,
    hen,
    inc,
    raw_s,
    score_s,
    mass_s,
    table,
    in_sem,
    small_sem,
    ssem,
    rsem,
):
    ny, nc, seqs, length = dims
    row = lax.axis_index("rows")
    me_c = lax.axis_index("cols")
    me_y, me_z = row // NZ, row % NZ

    def peer(axis, d):
        if axis == "z":
            return (me_y * NZ + (me_z + d) % NZ, me_c)
        if axis == "y":
            return (((me_y + d) % ny) * NZ + me_z, me_c)
        return (row, (me_c + d) % nc)

    size = {"z": NZ, "y": ny, "c": nc}
    mine = {"z": me_z, "y": me_y, "c": me_c}

    barrier = pltpu.get_barrier_semaphore()
    for axis in "yzc":
        for d in range(1, size[axis]):
            pl.semaphore_signal(barrier, inc=1, device_id=peer(axis, d), device_id_type=MESH)
    load = pltpu.make_async_copy(res_hbm, res_v, in_sem)
    load.start()
    small = [pltpu.make_async_copy(par_hbm, par_s, small_sem.at[0])]
    for copy in small:
        copy.start()

    def remote(src, dst, number, axis, d):
        return pltpu.make_async_remote_copy(
            src_ref=src,
            dst_ref=dst,
            send_sem=ssem.at[number, d - 1],
            recv_sem=rsem.at[number, d - 1],
            device_id=peer(axis, d),
            device_id_type=MESH,
        )

    def distances(axis):
        n = size[axis]
        return ORDER if n == 8 else tuple(range(1, n))

    def copies(buf, rows, number, axis):
        me = mine[axis]
        own = buf.at[me, pl.ds(0, rows)]
        return [remote(own, own, number, axis, d) for d in distances(axis)]

    def begin(made):
        for copy in made:
            copy.start()

    def arrive(made):
        for copy in made:
            copy.wait_recv()

    def leave(made):
        for copy in made:
            copy.wait_send()

    def total_of(buf, axis):
        s = buf[0]
        for i in range(1, size[axis]):
            s = s + buf[i]
        return s

    row16 = iota((16, LANES), 0)
    low16 = low((16, LANES))
    load.wait()

    for zd in range(NZ):
        block = pl.ds((zd // 2) * LANES, LANES)
        a, b = res_v[0:LANES, block], res_v[LANES : 2 * LANES, block]
        first = low((LANES, LANES))
        if zd % 2 == 0:
            stage[zd] = jnp.where(first, a, swap(b))
        else:
            stage[zd] = jnp.where(first, swap(a), b)

    def count_one(zd, carry):
        fields = [jnp.zeros((8, LANES), jnp.int32) for _ in range(5)]
        for t in range(LANES // 8):
            x = stage[zd, t * 8 : t * 8 + 8, :]
            unit = jnp.left_shift(jnp.ones((8, LANES), jnp.int32), (x & 3) * 8)
            which = x >> 2
            fields = [fields[q] + jnp.where(which == q, unit, 0) for q in range(5)]
        for q in range(5):
            v = fields[q]
            for step in (4, 2, 1):
                v = v + pltpu.roll(v, step, 0)
            for r in range(4):
                p = 4 * q + r
                line = ((v >> (8 * r)) & 255).astype(f32)
                if p < PAIRS:
                    cnt_lo[p : p + 1, :] = line[0:1]
                else:
                    cnt_hi[p - PAIRS : p - PAIRS + 1, :] = line[0:1]
        u, v = cnt_lo[...], cnt_hi[...]
        cnt_send[zd] = jnp.where(low16, u, v) + swap(jnp.where(low16, v, u))
        return carry

    lax.fori_loop(0, NZ, count_one, 0)
    cbuf[me_z] = cnt_send[me_z]
    held[me_z] = stage[me_z]

    pl.semaphore_wait(barrier, ny + NZ + nc - 3)

    sent_counts = []
    for d in distances("z"):
        other = (me_z + d) % NZ
        sent_counts.append(
            remote(cnt_send.at[other, pl.ds(0, PAIRS)], cbuf.at[me_z, pl.ds(0, PAIRS)], COUNT_Z, "z", d)
        )
    moved = [remote(stage.at[(me_z + d) % NZ], held.at[me_z], MOVE, "z", d) for d in distances("z")]
    begin(sent_counts)
    begin(moved)

    for b in range(NZ):
        half = (iota((16, LANES), 1) >= HALF).astype(jnp.int32)
        spread = jnp.where(row16 == 2 * b + half, 1.0, 0.0).astype(bf16)
        ones1[:, b * LANES : (b + 1) * LANES] = spread
        for n in range(3):
            ones3[16 * n : 16 * n + 16, b * LANES : (b + 1) * LANES] = spread
    low1 = low((1, LANES))
    for copy in small:
        copy.wait()
    for k in range(COMPONENTS):
        alpha[k] = jnp.ones((16, LANES), f32)
        for p in range(PAIRS):
            alpha[k, p : p + 1, :] = jnp.where(low1, par_s[k * ALPHABET + p], par_s[k * ALPHABET + p + PAIRS])
    inv_bg[...] = jnp.ones((16, LANES), f32)
    for p in range(PAIRS):
        inv_bg[p : p + 1, :] = jnp.where(low1, par_s[AT_BG + p], par_s[AT_BG + p + PAIRS])
    bg = inv_bg[...]
    inv_bg[...] = jnp.where(row16 < PAIRS, over_rows(fold(jnp.where(row16 < PAIRS, bg, 0.0))) / bg, 1.0)
    strength[...] = jnp.ones((16, LANES), f32)
    base[...] = jnp.zeros((16, LANES), f32)
    lik[...] = jnp.ones((16, LANES), f32)
    for k in range(COMPONENTS):
        al = alpha[k]
        strength[k : k + 1, :] = over_rows(fold(jnp.where(row16 < PAIRS, al, 0.0)))
        base[k : k + 1, :] = over_rows(fold(lgamma(al)))
        lik[k : k + 1, :] = jnp.where(low1, par_s[COMPONENTS * ALPHABET + k], par_s[COMPONENTS * ALPHABET + k])
    mix = lik[...]
    log_prior = jnp.log(mix) - jnp.log(over_rows(jnp.where(row16 < COMPONENTS, mix, 0.0)))
    base[...] = log_prior + lgamma(strength[...]) - base[...]

    arrive(sent_counts)
    ybuf[0, me_y] = total_of(cbuf, "z")
    ex = copies(ybuf.at[0], Y_ROWS, Y0, "y")
    begin(ex)
    arrive(ex)
    number = jnp.where(row16 < PAIRS, total_of(ybuf.at[0], "y"), 0.0)
    counts[...] = number
    gap = seqs - over_rows(fold(number))
    present = number > 0.5
    distinct = over_rows(fold(jnp.where(present, 1.0, 0.0))) + jnp.where(gap > 0.5, 1.0, 0.0)
    inverse = jnp.where(present, 1.0 / (distinct * jnp.maximum(number, 1.0)), 0.0)
    gap_inverse = jnp.where(gap > 0.5, 1.0 / (distinct * jnp.maximum(gap, 1.0)), 0.0)

    def set_table(lines, gap_line):
        other = swap(lines)
        table[0:PAIRS, :] = jnp.where(low16, lines, other)[0:PAIRS]
        table[PAIRS:ALPHABET, :] = jnp.where(low16, other, lines)[0:PAIRS]
        table[ALPHABET : ALPHABET + 1, :] = gap_line

    def sums_of_table(arriving=None):
        rows = [jnp.broadcast_to(table[a : a + 1, :], (16, LANES)) for a in range(ALPHABET + 1)]

        def look_up(b, at):
            v = pick(held[b, pl.ds(at, 16), :], rows)
            hi = v.astype(bf16)
            columns = pl.ds(b * LANES if isinstance(b, int) else pl.multiple_of(b * LANES, LANES), LANES)
            val_hi[pl.ds(at, 16), columns] = hi
            val_mid[pl.ds(at, 16), columns] = (v - hi.astype(f32)).astype(bf16)

        if arriving is None:

            def group(g, carry):
                for b in range(NZ):
                    look_up(b, pl.multiple_of(g * 16, 16))
                return carry

            lax.fori_loop(0, LANES // 16, group, 0)
        else:
            for b, copy in arriving:
                if copy is not None:
                    copy.wait_recv()

                def group(g, carry):
                    for u in range(4):
                        look_up(b, pl.multiple_of(g * 64 + u * 16, 16))
                    return carry

                lax.fori_loop(0, LANES // 64, group, 0)
        nt = (((1,), (1,)), ((), ()))
        e = ones1[...]
        return lax.dot_general(e, val_hi[...], nt, preferred_element_type=f32) + lax.dot_general(
            e, val_mid[...], nt, preferred_element_type=f32
        )

    def sum_over_columns(i, part, extra, meanwhile=None):
        zbuf[i, me_z, 0:16, :] = part
        zbuf[i, me_z, 16:24, :] = extra
        ex = copies(zbuf.at[i], S_ROWS, Z0 + i, "z")
        begin(ex)
        arrive(ex)
        sbuf[i, me_c] = total_of(zbuf.at[i], "z")
        ex = copies(sbuf.at[i], S_ROWS, C0 + i, "c")
        begin(ex)
        if meanwhile is not None:
            meanwhile()
        arrive(ex)
        return total_of(sbuf.at[i], "c")

    set_table(inverse, gap_inverse)
    arriving = [(me_z, None)]
    for d, copy in zip(distances("z"), moved):
        arriving.append(((me_z + NZ - d) % NZ, copy))
    hen[...] = sum_over_columns(0, sums_of_table(arriving), jnp.zeros((8, LANES), f32))[0:16] * (1.0 / length)
    inc[...] = jnp.ones((16, LANES), f32)

    def weighted_counts(i):
        def group(g, totals):
            for b in range(NZ):
                at = pl.multiple_of(g * 8, 8)
                x = held[b, pl.ds(at, 8), :]
                w = wide[pl.ds(at, 8), b * LANES : (b + 1) * LANES]
                totals = tuple(totals[a] + jnp.where(x == a, w, 0.0) for a in range(ALPHABET))
            return totals

        totals = lax.fori_loop(0, LANES // 8, group, tuple(jnp.zeros((8, LANES), f32) for _ in range(ALPHABET)))
        for p, line in enumerate(packed(totals)):
            ybuf[i, me_y, p : p + 1, :] = line

    def mixture(frequency):
        column_total = over_rows(fold(frequency))
        for k in range(COMPONENTS):
            lik[k : k + 1, :] = over_rows(lgamma(frequency + alpha[k]))
        lam = fold(lik[...]) + base[...] - lgamma(strength[...] + column_total)
        lam = jnp.where(row16 < COMPONENTS, lam, -1e30)
        e = jnp.exp(lam - jnp.max(lam, axis=0, keepdims=True))
        shares = e / (over_rows(e) * (column_total + strength[...]))
        smoothed = jnp.zeros((16, LANES), f32)
        for k in range(COMPONENTS):
            smoothed = smoothed + shares[k : k + 1, :] * (frequency + alpha[k])
        return jnp.log(smoothed * inv_bg[...])

    gathered = copies(pbuf, PAIRS, GATHER, "z")

    def finish_profile():
        arrive(gathered)
        for block in range(NZ // 2):
            even, odd = pbuf[2 * block], pbuf[2 * block + 1]
            at = pl.ds(block * LANES, LANES)
            prof_o[0:PAIRS, at] = jnp.where(low16, even, swap(odd))[0:PAIRS]
            prof_o[PAIRS:ALPHABET, at] = jnp.where(low16, swap(even), odd)[0:PAIRS]
        leave(sent_counts)
        leave(moved)
        leave(gathered)
        for i in range(ITERS + 1):
            leave(copies(ybuf.at[i], Y_ROWS, Y0 + i, "y"))
            leave(copies(zbuf.at[i], S_ROWS, Z0 + i, "z"))
            if i < ITERS:
                leave(copies(sbuf.at[i], S_ROWS, C0 + i, "c"))

    def iteration(it, carry):
        i = it + 1
        raw = hen[...] * inc[...]
        raw_s[...] = raw
        part_mass = jnp.broadcast_to(over_lanes(over_rows(raw)), (1, LANES))
        hi = raw.astype(bf16)
        rest = raw - hi.astype(f32)
        mid = rest.astype(bf16)
        pieces[0:16, :] = hi
        pieces[16:32, :] = mid
        pieces[32:48, :] = (rest - mid.astype(f32)).astype(bf16)
        wide[...] = lax.dot_general(
            pieces[...], ones3[...], (((0,), (0,)), ((), ())), preferred_element_type=f32
        )
        weighted_counts(i)
        ybuf[i, me_y, PAIRS : PAIRS + 1, :] = part_mass
        ex = copies(ybuf.at[i], Y_ROWS, Y0 + i, "y")
        begin(ex)
        arrive(ex)
        whole = total_of(ybuf.at[i], "y")
        mass = whole[PAIRS : PAIRS + 1, :]
        mass_s[...] = jnp.broadcast_to(mass, (8, LANES))
        frequency = jnp.where(row16 < PAIRS, whole, 0.0) * (COUNT_MASS / mass)
        profile = mixture(frequency)

        @pl.when(it == ITERS - 1)
        def _():
            pbuf[me_z] = profile
            begin(gathered)

        set_table(profile, jnp.zeros((1, LANES), f32))
        share = over_lanes(over_rows(jnp.where(row16 < PAIRS, profile * counts[...], 0.0)))
        extra = jnp.where(iota((8, LANES), 0) == 0, share, 0.0)
        done = sum_over_columns(i, sums_of_table(), extra, lambda: pl.when(it == ITERS - 1)(finish_profile))
        scores = done[0:16] * (1.0 / length)
        center = done[16:17, :] * (1.0 / (length * seqs))
        score_s[...] = scores
        inc[...] = 1.0 / (1.0 + jnp.exp((center - scores) * math.sqrt(length)))
        return carry

    lax.fori_loop(0, ITERS, iteration, 0)

    weights = raw_s[...] * (seqs / mass_s[0:1, :])
    scores = score_s[...]
    own_w, own_s = weights[0:2], scores[0:2]
    for b in range(1, NZ):
        own_w = jnp.where(me_z == b, weights[2 * b : 2 * b + 2], own_w)
        own_s = jnp.where(me_z == b, scores[2 * b : 2 * b + 2], own_s)
    line_o[0:2, :] = own_s
    line_o[2:4, :] = own_w

    leave(copies(sbuf.at[ITERS], S_ROWS, C0 + ITERS, "c"))


def solution(mesh):
    rows, cols = mesh.shape["rows"], mesh.shape["cols"]
    ny = rows // NZ

    def body(residues, dirichlet, mix_weight, background):
        high, across = residues.shape
        dims = (ny, cols, high * rows, across * cols)
        tile = pltpu.VMEM((16, LANES), f32)
        small = jnp.concatenate([dirichlet.reshape(-1), mix_weight, background])
        small = jnp.pad(small, (0, 256 - small.shape[0]))
        profile, lines = pl.pallas_call(
            functools.partial(kernel, dims),
            out_shape=(
                jax.ShapeDtypeStruct((ALPHABET, across), f32),
                jax.ShapeDtypeStruct((4, LANES), f32),
            ),
            in_specs=[
                pl.BlockSpec(memory_space=pl.ANY),
                pl.BlockSpec(memory_space=pl.ANY),
            ],
            out_specs=[pl.BlockSpec(memory_space=pltpu.VMEM)] * 2,
            scratch_shapes=[
                pltpu.SMEM((256,), f32),
                pltpu.VMEM((high, across), jnp.int32),
                pltpu.VMEM((NZ, LANES, LANES), jnp.int32),
                pltpu.VMEM((NZ, LANES, LANES), jnp.int32),
                pltpu.VMEM((NZ, 16, LANES), f32),
                tile,
                tile,
                pltpu.VMEM((NZ, 16, LANES), f32),
                pltpu.VMEM((ITERS + 1, ny, 16, LANES), f32),
                pltpu.VMEM((ITERS + 1, NZ, 24, LANES), f32),
                pltpu.VMEM((ITERS + 1, cols, 24, LANES), f32),
                pltpu.VMEM((NZ, 16, LANES), f32),
                pltpu.VMEM((LANES, NZ * LANES), f32),
                pltpu.VMEM((48, LANES), bf16),
                pltpu.VMEM((LANES, NZ * LANES), bf16),
                pltpu.VMEM((LANES, NZ * LANES), bf16),
                pltpu.VMEM((16, NZ * LANES), bf16),
                pltpu.VMEM((48, NZ * LANES), bf16),
                pltpu.VMEM((COMPONENTS, 16, LANES), f32),
                tile,
                tile,
                tile,
                tile,
                tile,
                tile,
                tile,
                tile,
                tile,
                pltpu.VMEM((8, LANES), f32),
                pltpu.VMEM((24, LANES), f32),
                pltpu.SemaphoreType.DMA,
                pltpu.SemaphoreType.DMA((3,)),
                pltpu.SemaphoreType.DMA((EXCHANGES, 7)),
                pltpu.SemaphoreType.DMA((EXCHANGES, 7)),
            ],
            compiler_params=pltpu.CompilerParams(
                collective_id=0, has_side_effects=True, vmem_limit_bytes=56_500_000
            ),
        )(residues, small)
        return profile, lines[0:2].reshape(-1), lines[2:4].reshape(-1)

    in_specs = (P("rows", "cols"), P(), P(), P())
    out_specs = (P(None, "cols"), P("rows"), P("rows"))
    return jax.shard_map(body, mesh=mesh, in_specs=in_specs, out_specs=out_specs, check_vma=False)
```
